32 devices in a mesh: groups: 1, expert: 32 (over z, y, x, core).
Axes of the slice: x: 2, y: 2, z: 4, core: 2. Of those that a mesh axis runs over, the one named last changes fastest.
Arguments:
- tokens: bfloat16 [256, 4096], P(('groups', 'expert')), may hold values from -400 to 400
- norm_gain: float32 [4096], replicated, may hold values from 0.1 to 1.9
- expert_ids: int32 [256, 8], P(('groups', 'expert')), may hold values from 0 to 15, all different within a row; in each aligned block of 8 rows (0 to 7, 8 to 15, ...) at most 5 rows name the same one
- route_score: float32 [256, 8], P(('groups', 'expert')), may hold values from 0.05 to 1
- expert_pair: int32 [16], P('groups'), may hold values from 0 to 15, each once
- w_in: bfloat16 [32, 4096, 768], P(('groups', 'expert')), may hold values from -0.09375 to 0.09375
- w_out: bfloat16 [32, 384, 4096], P(('groups', 'expert')), may hold values from -0.4375 to 0.4375
Outputs:
- mixed: bfloat16 [256, 4096], P(('groups', 'expert'))
The draws below stay inside these ranges and needn't reach their ends.
Inputs may be any that keep to these rules, and one draw needn't show every extreme that they name: `expert_ids`: each token names 8 different experts; among the tokens of one device no expert is named by more than 5 tokens, and in some devices' tokens one expert is named by exactly 5. `expert_pair`: each value once.
All inputs are finite; a program needn't handle non-finite values.
Results may differ from the reference program's by a relative error of at most 0.0076.
Values may be sent and summed in bfloat16 or wider, within the bound.
No kernel may reach another device: no remote copies, remote signals or barrier semaphores. Data moves between devices by JAX's collectives and lax.ppermute only.
A program may use at most 64 MiB of HBM per device.

```python
import math
import jax
import jax.numpy as jnp
import numpy as np
from jax import lax

D = 4096
EXPERT_FF = 768
TOP = 8
TOK_DEV = 8
HALF_FF = 384
EXPERTS = 16
TOKENS = 256
CAP = 5
N_EXPERT = 32


def draw_tokens(key, part):
    first, second, third = jax.random.split(key, 3)
    base = jnp.clip(jax.random.normal(first, (TOKENS, D), jnp.float32), -6.0, 6.0)
    scales = jnp.exp(jax.random.uniform(second, (TOKENS, 1), jnp.float32, 0.0, math.log(10.0)))
    columns = jnp.exp(jax.random.uniform(third, (1, D), jnp.float32, math.log(0.3), math.log(3.0)))
    return (base * scales * columns).astype(jnp.bfloat16)


def steps_of(key, extent, cuts, smallest, largest):
    gain, own = 1.0, jax.random.fold_in(key, 6)
    for dim, shards_of in cuts:
        draws = jnp.exp(jax.random.uniform(jax.random.fold_in(own, dim), (shards_of,), jnp.float32, smallest / len(cuts), largest / len(cuts)))
        gain = gain * jnp.repeat(draws, extent[dim] // shards_of).reshape([-1 if axis == dim else 1 for axis in range(len(extent))])
    return gain


def shared_out(rng, own, number, rows, amount, top, most, slope):
    ranking = jax.random.permutation(rng, amount)
    crowded, ordinary = portions_of(amount, rows * top, most, slope, True), portions_of(amount, rows * top, most, slope, False)
    places = jnp.arange(amount)

    def named(lengths, turn):
        used = int((lengths > 0).sum())
        fixed = max(1, used // 4)
        moved = fixed + (places - fixed + turn * (used - fixed)) % max(1, amount - fixed)
        return jnp.zeros((amount,), jnp.int32).at[ranking[jnp.where(places < fixed, places, moved)]].set(jnp.asarray(lengths, jnp.int32))

    lengths = jnp.where(number % 4 == 0, named(crowded, number // 4), named(ordinary, number - number // 4 - 1))
    mixed = jax.random.permutation(jax.random.fold_in(own, 3), amount)
    source_of, taker = mixed[0:amount // 2 * 2:2], mixed[1:amount // 2 * 2:2]
    room = jnp.minimum(lengths[source_of] - 1, most - lengths[taker]) // 2
    room = jnp.where((source_of == ranking[0]) | (taker == ranking[0]) | (lengths[taker] == 0), 0, jnp.maximum(room, 0))
    moved = jax.random.randint(jax.random.fold_in(own, 4), (amount // 2,), 0, 1 << 20) % (room + 1)
    lengths = lengths.at[source_of].add(-moved).at[taker].add(moved)
    items = jnp.searchsorted(jnp.cumsum(lengths), jnp.arange(rows * top), side="right").astype(jnp.int32)
    grid = items.reshape(top, rows).T
    grid = grid[jax.random.permutation(jax.random.fold_in(own, 1), rows)]
    turn = jax.random.randint(jax.random.fold_in(own, 2), (rows, 1), 0, top)
    return jnp.take_along_axis(grid, (jnp.arange(top)[None, :] + turn) % top, axis=1)


def portions_of(amount, total, bound, lean, full):
    weights = [(1 << 20) // math.isqrt(grade ** lean) + 1 for grade in range(1, amount + 1)]
    largest = bound if full else min(bound, max(-(-total // amount), total * weights[0] // sum(weights)))
    least = 1 if total - largest >= amount - 1 else 0
    given, spare = [largest] + [least] * (amount - 1), total - largest - least * (amount - 1)
    while spare > 0:
        movable = [i for i in range(1, amount) if given[i] < largest] or [i for i in range(1, amount) if given[i] < bound]
        whole, budget = sum([weights[i] for i in movable]), spare
        for i in movable:
            addition = min(bound - given[i], max(1, budget * weights[i] // whole), spare)
            given[i] = given[i] + addition
            spare = spare - addition
    return np.array(given)


def centred(key, extent, width, limit, cuts=(), kind=jnp.bfloat16):
    array = width * jax.random.normal(key, extent, jnp.float32)
    if cuts:
        array = array * steps_of(key, extent, cuts, -0.22, 0.18)
    return jnp.clip(array, -limit, limit).astype(kind)


def setup_inputs(seed: int = 0, part: int = 0) -> dict:
    key_of = jax.random.split(jax.random.key(seed), 8)
    part_splits = jax.random.split(jax.random.fold_in(key_of[7], part), 8)
    tokens = draw_tokens(jax.random.fold_in(jax.random.fold_in(key_of[7], part), 71), part)
    norm_gain = jnp.clip(1.0 + 0.18 * jax.random.normal(key_of[1], (D,), jnp.float32), 0.1, 1.9)
    expert_ids_keys = jax.random.split(jax.random.fold_in(part_splits[2], 1), TOKENS // TOK_DEV)
    expert_ids_turns = jax.random.permutation(jax.random.fold_in(part_splits[2], 3), TOKENS // TOK_DEV)
    expert_ids = jax.vmap(lambda own, number: shared_out(jax.random.fold_in(part_splits[2], 2), own, number, TOK_DEV, EXPERTS, TOP, CAP, 2))(expert_ids_keys, expert_ids_turns).reshape((TOKENS, TOP))
    route_score = jnp.clip(jnp.exp(math.log(1.0) - 2.9957323 * jax.random.uniform(part_splits[3], (TOKENS, TOP), jnp.float32) ** steps_of(part_splits[3], (TOKENS, TOP), ((0, 32),), -0.2, 0.2)), 0.05, 1.0)
    expert_pair = jax.random.permutation(part_splits[4], EXPERTS).astype(jnp.int32)
    w_in = centred(part_splits[5], (N_EXPERT, D, 2 * HALF_FF), D ** -0.5, 0.09375, ((0, 32),))
    w_out = centred(part_splits[6], (N_EXPERT, HALF_FF, D), (EXPERT_FF // 4) ** -0.5, 0.4375, ((0, 32),))
    return dict(tokens=tokens, norm_gain=norm_gain, expert_ids=expert_ids, route_score=route_score, expert_pair=expert_pair, w_in=w_in, w_out=w_out)


def reference(tokens, norm_gain, expert_ids, route_score, expert_pair, w_in, w_out):
    widened = tokens.astype(jnp.float32)
    meansq = lax.optimization_barrier(jnp.mean(widened * widened, axis=-1, keepdims=True))
    normed = (widened * lax.rsqrt(meansq + 1e-06) * norm_gain).astype(jnp.bfloat16)
    shares = (route_score / lax.optimization_barrier(jnp.sum(route_score, axis=-1, keepdims=True))).astype(jnp.bfloat16)
    half_units = w_out.shape[1]
    row_limit = N_EXPERT * CAP
    labels = jnp.arange(EXPERTS, dtype=jnp.int32)

    def expert_step(totals, expert):
        station = jnp.sum(jnp.where(labels == expert, expert_pair, 0)).astype(jnp.int32)
        inward = lax.dynamic_slice_in_dim(w_in, 2 * station, 2, 0)
        outward = lax.dynamic_slice_in_dim(w_out, 2 * station, 2, 0).reshape(2 * half_units, D)
        gate_full = jnp.concatenate([inward[0, :, :half_units], inward[1, :, :half_units]], axis=1)
        up_full = jnp.concatenate([inward[0, :, half_units:], inward[1, :, half_units:]], axis=1)
        chosen = expert_ids == expert
        members = jnp.nonzero(jnp.any(chosen, axis=-1), size=row_limit, fill_value=TOKENS)[0].astype(jnp.int32)
        inputs = jnp.take(normed, members, axis=0, mode='fill', fill_value=0)
        gate_val = jnp.dot(inputs, gate_full, preferred_element_type=jnp.float32)
        up_val = jnp.dot(inputs, up_full, preferred_element_type=jnp.float32)
        hidden = (jax.nn.silu(gate_val) * up_val).astype(jnp.bfloat16)
        result = jnp.dot(hidden, outward, preferred_element_type=jnp.float32).astype(jnp.bfloat16)
        token_weight = lax.optimization_barrier(jnp.sum(jnp.where(chosen, shares.astype(jnp.float32), 0.0), axis=-1))
        row_weight = jnp.take(token_weight, members, mode='fill', fill_value=0)
        totals = totals.at[members].add(row_weight[:, None] * result.astype(jnp.float32), mode='drop')
        return (totals, None)
    totals = lax.scan(expert_step, jnp.zeros((TOKENS, D), jnp.float32), labels)[0]
    return totals.astype(jnp.bfloat16)
```

```python
import functools

import jax
import jax.numpy as jnp
from jax import lax
from jax.experimental import pallas as pl
from jax.experimental.pallas import tpu as pltpu
from jax.sharding import PartitionSpec as P


LANES = 128
BF16 = jnp.bfloat16
F32 = jnp.float32
VMEM = pl.BlockSpec(memory_space=pltpu.VMEM)
SMEM = pl.BlockSpec(memory_space=pltpu.SMEM)
ANY = pl.BlockSpec(memory_space=pl.ANY)


def swap(block, mask):
    count = lax.axis_size("expert")
    return lax.ppermute(block, "expert", [(i, i ^ mask) for i in range(count)])


def prepare_kernel(tokens, gain, ids, score, pair, payload, *, width):
    widened = tokens[...].astype(F32)
    meansq = jnp.mean(widened * widened, axis=-1, keepdims=True)
    normed = widened * lax.rsqrt(meansq + 1e-06) * gain[...]
    payload[:, :width] = normed.astype(BF16)
    rows, top = ids.shape
    stations = pair.shape[1]
    table = payload.shape[1] - width
    shares = score[...] / jnp.sum(score[...], axis=-1, keepdims=True)
    labels = lax.broadcasted_iota(jnp.int32, (rows, stations), 1)
    named = jnp.zeros((rows, stations), F32)
    for k in range(top):
        named = named + jnp.where(ids[:, k : k + 1] == labels, shares[:, k : k + 1], 0.0)
    place = lax.broadcasted_iota(jnp.int32, (table, stations), 0)
    moved = jnp.where(pair[...] == place, 1.0, 0.0).astype(BF16)
    payload[:, width:] = lax.dot_general(
        named.astype(BF16), moved, (((1,), (1,)), ((), ())), preferred_element_type=F32
    ).astype(BF16)


def select_kernel(station, *refs, blocks, peers, cap, slots, width):
    payloads = refs[:blocks]
    own, weights = refs[blocks : blocks + 2]
    chosen = refs[blocks + 2 :]
    rows_each = payloads[0].shape[0]
    rows = blocks * rows_each
    gathered = jnp.concatenate([ref[...].astype(F32) for ref in payloads], axis=0)
    table = gathered[:, width:]
    body = gathered[:, :width].astype(BF16)
    own[...] = body
    named = jnp.where(table > 0.0, 1.0, 0.0)
    row = lax.broadcasted_iota(jnp.int32, (rows, rows), 0)
    col = lax.broadcasted_iota(jnp.int32, (rows, rows), 1)
    earlier = (col < row) & (row // rows_each == col // rows_each)
    rank = jnp.dot(
        jnp.where(earlier, 1.0, 0.0).astype(BF16), named.astype(BF16), preferred_element_type=F32
    )
    block = lax.broadcasted_iota(jnp.int32, (rows, 1), 0) // rows_each
    lane = lax.broadcasted_iota(jnp.int32, (rows, table.shape[1]), 1)
    total = weights.shape[1]
    target = lax.broadcasted_iota(jnp.int32, (rows, total), 1)
    shared = jnp.zeros((rows, total), F32)
    for j in range(peers + 1):
        pick = lane == (station[0] ^ j)
        share = jnp.sum(jnp.where(pick, table, 0.0), axis=1, keepdims=True)
        if j == 0:
            slot = lax.broadcasted_iota(jnp.int32, (rows, 1), 0)
        else:
            ranked = jnp.sum(jnp.where(pick, rank, 0.0), axis=1, keepdims=True)
            slot = block * cap + ranked.astype(jnp.int32) + (rows + (j - 1) * slots)
        shared = shared + jnp.where(target == slot, share, 0.0)
    weights[...] = shared.astype(BF16)
    placing = jnp.where(shared[:, rows:] > 0.0, 1.0, 0.0).astype(BF16)
    picked = lax.dot_general(
        placing, body, (((0,), (0,)), ((), ())), preferred_element_type=F32
    )
    for j in range(peers):
        chosen[j][...] = picked[j * slots : (j + 1) * slots].astype(BF16)


def expert_kernel(*refs, pieces, steps_in, steps_out):
    inputs = refs[:pieces]
    w_in, w_out = refs[pieces : pieces + 2]
    keep, give = refs[pieces + 2 : pieces + 4]
    stacked, inward, outward, acc, in_sem, out_sem = refs[pieces + 4 :]
    width, units = w_in.shape[1:]
    half = units // 2
    k_len = width // steps_in
    n_len = width // steps_out
    copies_in = [
        pltpu.make_async_copy(
            w_in.at[0, pl.ds(s * k_len, k_len)], inward.at[pl.ds(s * k_len, k_len)], in_sem.at[s]
        )
        for s in range(steps_in)
    ]
    copy_out = pltpu.make_async_copy(w_out.at[0], outward, out_sem)
    for copy in copies_in:
        copy.start()
    copy_out.start()
    offset = 0
    for ref in inputs:
        stacked[offset : offset + ref.shape[0]] = ref[...]
        offset += ref.shape[0]
    for s in range(steps_in):
        copies_in[s].wait()
        part = jnp.dot(
            stacked[:, s * k_len : (s + 1) * k_len],
            inward[s * k_len : (s + 1) * k_len],
            preferred_element_type=F32,
        )
        if s == 0:
            acc[...] = part
        else:
            acc[...] += part
    gate = acc[:, :half]
    hidden = (gate / (1.0 + jnp.exp(-gate)) * acc[:, half:]).astype(BF16)
    copy_out.wait()
    rows = keep.shape[0]
    for s in range(steps_out):
        cols = slice(s * n_len, (s + 1) * n_len)
        value = jnp.dot(hidden, outward[:, cols], preferred_element_type=F32)
        keep[:, cols] = value[:rows]
        give[:, cols] = value[rows:].astype(BF16)


def finish_kernel(keep, got, own, *sent):
    rows = own.shape[0]
    own[...] = (keep[:rows] + got[:rows].astype(F32)).astype(BF16)
    offset = rows
    for ref in sent:
        end = offset + ref.shape[0]
        ref[...] = (keep[offset:end] + got[offset:end].astype(F32)).astype(BF16)
        offset = end


def combine_kernel(weights, own, *refs, peers):
    back = refs[:peers]
    blocks = refs[peers:]
    stacked = jnp.concatenate([own[...]] + [ref[...] for ref in back], axis=0)
    mixed = jnp.dot(weights[:, : stacked.shape[0]], stacked, preferred_element_type=F32)
    rows = blocks[0].shape[0]
    for b, ref in enumerate(blocks):
        ref[...] = mixed[b * rows : (b + 1) * rows].astype(ref.dtype)


def total_kernel(first, *refs):
    total = first[...]
    for ref in refs[:-1]:
        total = total + ref[...].astype(F32)
    refs[-1][...] = total.astype(BF16)


def call(kernel, ins, outs, scratch=(), **kwargs):
    return pl.pallas_call(
        kernel,
        in_specs=list(ins),
        out_specs=[VMEM] * len(outs),
        out_shape=[jax.ShapeDtypeStruct(*out) for out in outs],
        scratch_shapes=list(scratch),
        **kwargs,
    )


def on_device(tokens, norm_gain, expert_ids, route_score, expert_pair, w_in, w_out):
    devices = lax.axis_size("expert")
    chips = devices // 2
    bits = chips.bit_length() - 1
    low = bits // 2
    plane = 1 << low
    blocks = chips // plane
    peers = plane - 1
    stations = expert_pair.shape[0]
    rows, top = expert_ids.shape
    width = tokens.shape[1]
    cap = min(rows, -(-rows * top // stations) + 1)
    slots = -(-blocks * cap // 8) * 8
    table = -(-stations // LANES) * LANES
    held = blocks * rows
    local = held + peers * slots
    station = (lax.axis_index("expert") // 2).astype(jnp.int32).reshape(1)

    (payload,) = call(
        functools.partial(prepare_kernel, width=width),
        [VMEM] * 5,
        [((rows, width + table), BF16)],
    )(tokens, norm_gain.reshape(1, width), expert_ids, route_score, expert_pair.reshape(1, stations))

    column = [payload] + [swap(payload, k << (low + 1)) for k in range(1, blocks)]
    own, weights, *chosen = call(
        functools.partial(
            select_kernel, blocks=blocks, peers=peers, cap=cap, slots=slots, width=width
        ),
        [SMEM] + [VMEM] * blocks,
        [((held, width), BF16), ((held, local), BF16)] + [((slots, width), BF16)] * peers,
    )(station, *column)

    arrived = [swap(chosen[j - 1], j << 1) for j in range(1, plane)]
    own_other = swap(own, 1)
    arrived_other = [swap(block, 1) for block in arrived]
    pieces = [own] + arrived + [own_other] + arrived_other
    half = w_out.shape[1]
    steps_in, steps_out = 8, 4
    keep, give = call(
        functools.partial(
            expert_kernel, pieces=len(pieces), steps_in=steps_in, steps_out=steps_out
        ),
        [VMEM] * len(pieces) + [ANY, ANY],
        [((local, width), F32), ((local, width), BF16)],
        [
            pltpu.VMEM((2 * local, width), BF16),
            pltpu.VMEM((width, 2 * half), BF16),
            pltpu.VMEM((half, width), BF16),
            pltpu.VMEM((2 * local, 2 * half), F32),
            pltpu.SemaphoreType.DMA((steps_in,)),
            pltpu.SemaphoreType.DMA,
        ],
    )(*pieces, w_in, w_out)

    got = swap(give, 1)
    own_done, *sent = call(
        finish_kernel,
        [VMEM] * 2,
        [((held, width), BF16)] + [((slots, width), BF16)] * peers,
    )(keep, got)
    back = [swap(sent[j - 1], j << 1) for j in range(1, plane)]
    summed = call(
        functools.partial(combine_kernel, peers=peers),
        [VMEM] * (2 + peers),
        [((rows, width), F32)] + [((rows, width), BF16)] * (blocks - 1),
    )(weights, own_done, *back)
    returned = [swap(summed[k], k << (low + 1)) for k in range(1, blocks)]
    (mixed,) = call(total_kernel, [VMEM] * blocks, [((rows, width), BF16)])(summed[0], *returned)
    return mixed


def solution(mesh):
    in_specs = (
        P(("groups", "expert"), None),
        P(),
        P(("groups", "expert"), None),
        P(("groups", "expert"), None),
        P("groups"),
        P(("groups", "expert"), None, None),
        P(("groups", "expert"), None, None),
    )
    out_specs = P(("groups", "expert"), None)
    return jax.shard_map(
        on_device, mesh=mesh, in_specs=in_specs, out_specs=out_specs, check_vma=False
    )
```

```python
import functools

import jax
import jax.numpy as jnp
from jax import lax
from jax.experimental import pallas as pl
from jax.experimental.pallas import tpu as pltpu
from jax.sharding import PartitionSpec as P


LANES = 128
BF16 = jnp.bfloat16
F32 = jnp.float32
HBM = pl.BlockSpec(memory_space=pltpu.HBM)
VMEM = pl.BlockSpec(memory_space=pltpu.VMEM)
SMEM = pl.BlockSpec(memory_space=pltpu.SMEM)


def swap(block, mask):
    count = lax.axis_size("expert")
    return lax.ppermute(block, "expert", [(i, i ^ mask) for i in range(count)])


def prepare_kernel(tokens, gain, ids, score, pair, payload, *, width):
    widened = tokens[...].astype(F32)
    meansq = jnp.mean(widened * widened, axis=-1, keepdims=True)
    normed = widened * lax.rsqrt(meansq + 1e-06) * gain[...]
    payload[:, :width] = normed.astype(BF16)
    rows, top = ids.shape
    stations = pair.shape[1]
    table = payload.shape[1] - width
    shares = score[...] / jnp.sum(score[...], axis=-1, keepdims=True)
    labels = lax.broadcasted_iota(jnp.int32, (rows, stations), 1)
    named = jnp.zeros((rows, stations), F32)
    for k in range(top):
        named = named + jnp.where(ids[:, k : k + 1] == labels, shares[:, k : k + 1], 0.0)
    place = lax.broadcasted_iota(jnp.int32, (table, stations), 0)
    moved = jnp.where(pair[...] == place, 1.0, 0.0).astype(BF16)
    payload[:, width:] = lax.dot_general(
        named.astype(BF16), moved, (((1,), (1,)), ((), ())), preferred_element_type=F32
    ).astype(BF16)


def select_kernel(station, *refs, blocks, peers, cap, slots, width):
    payloads = refs[:blocks]
    own, shares, weights = refs[blocks : blocks + 3]
    chosen = refs[blocks + 3 :]
    rows_each = payloads[0].shape[0]
    rows = blocks * rows_each
    gathered = jnp.concatenate([ref[...].astype(F32) for ref in payloads], axis=0)
    table = gathered[:, width:]
    body = gathered[:, :width].astype(BF16)
    own[...] = body
    named = jnp.where(table > 0.0, 1.0, 0.0)
    row = lax.broadcasted_iota(jnp.int32, (rows, rows), 0)
    col = lax.broadcasted_iota(jnp.int32, (rows, rows), 1)
    earlier = (col < row) & (row // rows_each == col // rows_each)
    rank = jnp.dot(
        jnp.where(earlier, 1.0, 0.0).astype(BF16), named.astype(BF16), preferred_element_type=F32
    )
    block = lax.broadcasted_iota(jnp.int32, (rows, 1), 0) // rows_each
    lane = lax.broadcasted_iota(jnp.int32, (rows, table.shape[1]), 1)
    total = weights.shape[1]
    target = lax.broadcasted_iota(jnp.int32, (rows, total), 1)
    shared = jnp.zeros((rows, total), F32)
    for j in range(peers + 1):
        pick = lane == (station[0] ^ j)
        share = jnp.sum(jnp.where(pick, table, 0.0), axis=1, keepdims=True)
        if j == 0:
            shares[...] = jnp.broadcast_to(share, shares.shape)
            continue
        ranked = jnp.sum(jnp.where(pick, rank, 0.0), axis=1, keepdims=True)
        slot = block * cap + ranked.astype(jnp.int32) + (j - 1) * slots
        shared = shared + jnp.where(target == slot, share, 0.0)
    weights[...] = shared.astype(BF16)
    placing = jnp.where(shared > 0.0, 1.0, 0.0).astype(BF16)
    picked = lax.dot_general(
        placing, body, (((0,), (0,)), ((), ())), preferred_element_type=F32
    )
    for j in range(peers):
        chosen[j][...] = picked[j * slots : (j + 1) * slots].astype(BF16)


def activate(projected):
    half = projected.shape[1] // 2
    gate = projected[:, :half]
    return (gate / (1.0 + jnp.exp(-gate)) * projected[:, half:]).astype(BF16)


def own_kernel(
    own, other, w_in, w_out, keep, give, inward, outward, stacked, acc, in_sem, out_sem, *, steps_in, steps_out
):
    rows, width = own.shape
    k_len = width // steps_in
    n_len = width // steps_out
    copies_in = [
        pltpu.make_async_copy(
            w_in.at[0, pl.ds(s * k_len, k_len)], inward.at[pl.ds(s * k_len, k_len)], in_sem.at[s]
        )
        for s in range(steps_in)
    ]
    copy_out = pltpu.make_async_copy(w_out.at[0], outward, out_sem)
    for copy in copies_in:
        copy.start()
    copy_out.start()
    stacked[:rows] = own[...]
    stacked[rows:] = other[...]
    for s in range(steps_in):
        span = slice(s * k_len, (s + 1) * k_len)
        copies_in[s].wait()
        part = jnp.dot(stacked[:, span], inward[span], preferred_element_type=F32)
        if s == 0:
            acc[...] = part
        else:
            acc[...] += part
    hidden = activate(acc[...])
    copy_out.wait()
    for s in range(steps_out):
        cols = slice(s * n_len, (s + 1) * n_len)
        value = jnp.dot(hidden, outward[:, cols], preferred_element_type=F32)
        keep[:, cols] = value[:rows]
        give[:, cols] = value[rows:].astype(BF16)


def peer_kernel(*refs, peers, steps_out):
    pieces = refs[: 2 * peers]
    inward, outward = refs[2 * peers : 2 * peers + 2]
    results = refs[2 * peers + 2 : 4 * peers + 2]
    stacked = refs[-1]
    slots, width = pieces[0].shape
    for p, ref in enumerate(pieces):
        stacked[p * slots : (p + 1) * slots] = ref[...]
    hidden = activate(jnp.dot(stacked[...], inward[...], preferred_element_type=F32))
    n_len = width // steps_out
    for s in range(steps_out):
        cols = slice(s * n_len, (s + 1) * n_len)
        value = jnp.dot(hidden, outward[:, cols], preferred_element_type=F32)
        for p, ref in enumerate(results):
            ref[:, cols] = value[p * slots : (p + 1) * slots].astype(ref.dtype)


def combine_kernel(shares, weights, keep, got, *refs, peers):
    back = refs[:peers]
    blocks = refs[peers:]
    stacked = jnp.concatenate([ref[...] for ref in back], axis=0)
    mixed = jnp.dot(weights[...], stacked, preferred_element_type=F32)
    mixed = mixed + shares[:, :1] * (keep[...] + got[...].astype(F32))
    rows = blocks[0].shape[0]
    for b, ref in enumerate(blocks):
        ref[...] = mixed[b * rows : (b + 1) * rows].astype(ref.dtype)


def call(kernel, ins, outs, scratch=(), limit=6, flops=0, moved=0):
    return pl.pallas_call(
        kernel,
        in_specs=list(ins),
        out_specs=[VMEM] * len(outs),
        out_shape=[jax.ShapeDtypeStruct(*out) for out in outs],
        scratch_shapes=list(scratch),
        cost_estimate=pl.CostEstimate(flops=flops, bytes_accessed=moved, transcendentals=0),
        compiler_params=pltpu.CompilerParams(vmem_limit_bytes=limit << 20),
    )


def layer(tokens, norm_gain, expert_ids, route_score, expert_pair, w_in, w_out):
    devices = lax.axis_size("expert")
    chips = devices // 2
    bits = chips.bit_length() - 1
    low = bits // 2
    plane = 1 << low
    blocks = chips // plane
    peers = plane - 1
    stations = expert_pair.shape[0]
    rows, top = expert_ids.shape
    width = tokens.shape[1]
    cap = min(rows, -(-rows * top // stations) + 1)
    slots = -(-blocks * cap // 8) * 8
    table = -(-stations // LANES) * LANES
    held = blocks * rows
    half = w_out.shape[1]
    steps_in, steps_out = 8, 4
    station = (lax.axis_index("expert") // 2).astype(jnp.int32).reshape(1)

    (payload,) = call(
        functools.partial(prepare_kernel, width=width),
        [VMEM] * 5,
        [((rows, width + table), BF16)],
    )(tokens, norm_gain.reshape(1, width), expert_ids, route_score, expert_pair.reshape(1, stations))

    column = [payload] + [swap(payload, k << (low + 1)) for k in range(1, blocks)]
    own, shares, weights, *chosen = call(
        functools.partial(
            select_kernel, blocks=blocks, peers=peers, cap=cap, slots=slots, width=width
        ),
        [SMEM] + [VMEM] * blocks,
        [((held, width), BF16), ((held, LANES), F32), ((held, peers * slots), BF16)]
        + [((slots, width), BF16)] * peers,
    )(station, *column)

    arrived = []
    for j in range(1, plane):
        arrived.append(swap(chosen[j - 1], j << 1))
    other = swap(own, 1)
    keep, give, inward, outward = call(
        functools.partial(own_kernel, steps_in=steps_in, steps_out=steps_out),
        [VMEM, VMEM, HBM, HBM],
        [
            ((held, width), F32),
            ((held, width), BF16),
            ((width, 2 * half), BF16),
            ((half, width), BF16),
        ],
        [
            pltpu.VMEM((2 * held, width), BF16),
            pltpu.VMEM((2 * held, 2 * half), F32),
            pltpu.SemaphoreType.DMA((steps_in,)),
            pltpu.SemaphoreType.DMA,
        ],
        flops=2400 * held * half * width,
    )(
        own,
        other,
        pltpu.with_memory_space_constraint(w_in, pltpu.HBM),
        pltpu.with_memory_space_constraint(w_out, pltpu.HBM),
    )
    got = swap(give, 1)

    pieces = arrived + [swap(block, 1) for block in arrived]
    results = call(
        functools.partial(peer_kernel, peers=peers, steps_out=steps_out),
        [VMEM] * (2 * peers + 2),
        [((slots, width), F32)] * peers + [((slots, width), BF16)] * peers,
        [pltpu.VMEM((2 * peers * slots, width), BF16)],
        limit=12,
    )(*pieces, inward, outward)
    back = []
    for j in range(peers):
        done = results[j] + swap(results[peers + j], 1).astype(F32)
        back.append(swap(done.astype(BF16), (j + 1) << 1))

    summed = call(
        functools.partial(combine_kernel, peers=peers),
        [VMEM] * (4 + peers),
        [((rows, width), F32)] + [((rows, width), BF16)] * (blocks - 1),
    )(shares, weights, keep, got, *back)
    mixed = summed[0]
    for k in range(1, blocks):
        mixed = mixed + swap(summed[k], k << (low + 1)).astype(F32)
    mixed = mixed.astype(BF16)
    return mixed


def solution(mesh):
    in_specs = (
        P(("groups", "expert"), None),
        P(),
        P(("groups", "expert"), None),
        P(("groups", "expert"), None),
        P("groups"),
        P(("groups", "expert"), None, None),
        P(("groups", "expert"), None, None),
    )
    out_specs = P(("groups", "expert"), None)
    return jax.shard_map(layer, mesh=mesh, in_specs=in_specs, out_specs=out_specs, check_vma=False)
```

```python
import functools

import jax
import jax.numpy as jnp
from jax import lax
from jax.experimental import pallas as pl
from jax.experimental.pallas import tpu as pltpu
from jax.sharding import PartitionSpec as P


LANES = 128
BF16 = jnp.bfloat16
F32 = jnp.float32
HBM = pl.BlockSpec(memory_space=pltpu.HBM)
VMEM = pl.BlockSpec(memory_space=pltpu.VMEM)
SMEM = pl.BlockSpec(memory_space=pltpu.SMEM)


def swap(block, mask):
    count = lax.axis_size("expert")
    return lax.ppermute(block, "expert", [(i, i ^ mask) for i in range(count)])


def picked_rows(placing, body):
    return lax.dot_general(placing, body, (((0,), (0,)), ((), ())), preferred_element_type=F32)


def slot_weights(table, station, peers, slots, cap, rows_each):
    rows = table.shape[0]
    row = lax.broadcasted_iota(jnp.int32, (rows, rows), 0)
    col = lax.broadcasted_iota(jnp.int32, (rows, rows), 1)
    earlier = (col < row) & (row // rows_each == col // rows_each)
    rank = jnp.dot(
        jnp.where(earlier, 1.0, 0.0).astype(BF16),
        jnp.where(table > 0.0, 1.0, 0.0).astype(BF16),
        preferred_element_type=F32,
    )
    base = lax.broadcasted_iota(jnp.int32, (rows, 1), 0) // rows_each * cap
    lane = lax.broadcasted_iota(jnp.int32, table.shape, 1)
    target = lax.broadcasted_iota(jnp.int32, (rows, peers * slots), 1)
    weights = jnp.zeros((rows, peers * slots), F32)
    for j in range(peers):
        pick = lane == (station ^ (j + 1))
        share = jnp.sum(jnp.where(pick, table, 0.0), axis=1, keepdims=True)
        ranked = jnp.sum(jnp.where(pick, rank, 0.0), axis=1, keepdims=True)
        slot = base + ranked.astype(jnp.int32) + j * slots
        weights = weights + jnp.where(target == slot, share, 0.0)
    return weights


def prepare_kernel(station, *refs, peers, cap, slots, width):
    sources = refs[:5]
    payload, weights = refs[5:7]
    chosen = refs[7 : 7 + peers]
    copied = refs[7 + peers : 12 + peers]
    sems = refs[-1]
    copies = [
        pltpu.make_async_copy(source, target, sems.at[n])
        for n, (source, target) in enumerate(zip(sources, copied))
    ]
    for copy in copies:
        copy.start()
    for copy in copies:
        copy.wait()
    tokens, gain, ids, score, pair = copied
    widened = tokens[...].astype(F32)
    meansq = jnp.mean(widened * widened, axis=-1, keepdims=True)
    normed = (widened * lax.rsqrt(meansq + 1e-06) * gain[...]).astype(BF16)
    payload[:, :width] = normed
    rows, top = ids.shape
    stations = pair.shape[1]
    shares = score[...] / jnp.sum(score[...], axis=-1, keepdims=True)
    labels = lax.broadcasted_iota(jnp.int32, (rows, stations), 1)
    named = jnp.zeros((rows, stations), F32)
    for k in range(top):
        named = named + jnp.where(ids[:, k : k + 1] == labels, shares[:, k : k + 1], 0.0)
    place = lax.broadcasted_iota(jnp.int32, (payload.shape[1] - width, stations), 0)
    moved = jnp.where(pair[...] == place, 1.0, 0.0).astype(BF16)
    table = lax.dot_general(
        named.astype(BF16), moved, (((1,), (1,)), ((), ())), preferred_element_type=F32
    )
    payload[:, width:] = table.astype(BF16)
    shared = slot_weights(table, station[0], peers, slots, cap, rows)
    weights[...] = shared.astype(BF16)
    placed = picked_rows(jnp.where(shared > 0.0, 1.0, 0.0).astype(BF16), normed)
    for j, ref in enumerate(chosen):
        ref[...] = placed[j * slots : (j + 1) * slots].astype(BF16)


def select_kernel(station, *refs, blocks, peers, cap, slots, width):
    payloads = refs[:blocks]
    own, shares, weights = refs[blocks : blocks + 3]
    chosen = refs[blocks + 3 :]
    rows = payloads[0].shape[0]
    gathered = jnp.concatenate([ref[...].astype(F32) for ref in payloads], axis=0)
    table = gathered[:, width:]
    body = gathered[:, :width].astype(BF16)
    own[...] = body
    lane = lax.broadcasted_iota(jnp.int32, table.shape, 1)
    share = jnp.sum(jnp.where(lane == station[0], table, 0.0), axis=1, keepdims=True)
    shares[...] = jnp.broadcast_to(share, shares.shape)
    shared = slot_weights(table[rows:], station[0], peers, slots, cap, rows)
    weights[...] = shared.astype(BF16)
    placed = picked_rows(jnp.where(shared > 0.0, 1.0, 0.0).astype(BF16), body[rows:])
    for j, ref in enumerate(chosen):
        ref[...] = placed[j * slots : (j + 1) * slots].astype(BF16)


def activate(projected):
    half = projected.shape[1] // 2
    gate = projected[:, :half]
    return (gate / (1.0 + jnp.exp(-gate)) * projected[:, half:]).astype(BF16)


def own_kernel(
    own, other, w_in, w_out, keep, give, inward, outward, stacked, acc, in_sem, out_sem, *, steps_in, steps_out
):
    rows, width = own.shape
    k_len = width // steps_in
    n_len = width // steps_out
    copies_in = [
        pltpu.make_async_copy(
            w_in.at[0, pl.ds(s * k_len, k_len)], inward.at[pl.ds(s * k_len, k_len)], in_sem.at[s]
        )
        for s in range(steps_in)
    ]
    copy_out = pltpu.make_async_copy(w_out.at[0], outward, out_sem)
    for copy in copies_in:
        copy.start()
    copy_out.start()
    stacked[:rows] = own[...]
    stacked[rows:] = other[...]
    for s in range(steps_in):
        span = slice(s * k_len, (s + 1) * k_len)
        copies_in[s].wait()
        part = jnp.dot(stacked[:, span], inward[span], preferred_element_type=F32)
        if s == 0:
            acc[...] = part
        else:
            acc[...] += part
    hidden = activate(acc[...])
    copy_out.wait()
    for s in range(steps_out):
        cols = slice(s * n_len, (s + 1) * n_len)
        value = jnp.dot(hidden, outward[:, cols], preferred_element_type=F32)
        keep[:, cols] = value[:rows]
        give[:, cols] = value[rows:].astype(BF16)


def peer_kernel(*refs, peers, steps_out):
    pieces = refs[: 2 * peers]
    inward, outward = refs[2 * peers : 2 * peers + 2]
    results = refs[2 * peers + 2 : 4 * peers + 2]
    stacked = refs[-1]
    slots, width = pieces[0].shape
    for p, ref in enumerate(pieces):
        stacked[p * slots : (p + 1) * slots] = ref[...]
    hidden = activate(jnp.dot(stacked[...], inward[...], preferred_element_type=F32))
    n_len = width // steps_out
    for s in range(steps_out):
        cols = slice(s * n_len, (s + 1) * n_len)
        value = jnp.dot(hidden, outward[:, cols], preferred_element_type=F32)
        for p, ref in enumerate(results):
            ref[:, cols] = value[p * slots : (p + 1) * slots].astype(ref.dtype)


def combine_kernel(shares, weights, keep, got, *refs, peers):
    back = refs[:peers]
    blocks = refs[peers:]
    stacked = jnp.concatenate([ref[...] for ref in back], axis=0)
    mixed = jnp.dot(weights[...], stacked, preferred_element_type=F32)
    held = shares.shape[0]
    local = shares[:, :1] * (keep[:held] + got[:held].astype(F32))
    rows = blocks[0].shape[0]
    blocks[0][...] = local[:rows]
    for b, ref in enumerate(blocks[1:]):
        span = slice(b * rows, (b + 1) * rows)
        ref[...] = (mixed[span] + local[rows:][span]).astype(BF16)


def total_kernel(local, weights, *refs, peers):
    back = refs[:peers]
    stacked = jnp.concatenate([ref[...] for ref in back], axis=0)
    total = local[...] + jnp.dot(weights[...], stacked, preferred_element_type=F32)
    for ref in refs[peers:-1]:
        total = total + ref[...].astype(F32)
    refs[-1][...] = total.astype(BF16)


def call(kernel, ins, outs, scratch=(), limit=6, flops=0, moved=0):
    return pl.pallas_call(
        kernel,
        in_specs=list(ins),
        out_specs=[VMEM] * len(outs),
        out_shape=[jax.ShapeDtypeStruct(*out) for out in outs],
        scratch_shapes=list(scratch),
        cost_estimate=pl.CostEstimate(flops=flops, bytes_accessed=moved, transcendentals=0),
        compiler_params=pltpu.CompilerParams(vmem_limit_bytes=limit << 20),
    )


def layer(tokens, norm_gain, expert_ids, route_score, expert_pair, w_in, w_out):
    devices = lax.axis_size("expert")
    blocks, plane, up = shape_of(devices)
    peers = plane - 1
    stations = expert_pair.shape[0]
    rows, top = expert_ids.shape
    width = tokens.shape[1]
    half = w_out.shape[1]
    cap = min(rows, -(-rows * top // stations) + 1)
    slots_first = -(-cap // 8) * 8
    slots = -(-(blocks - 1) * cap // 8) * 8
    table = -(-stations // LANES) * LANES
    held = blocks * rows
    early = held + peers * slots_first
    steps_in, steps_out = 8, 4
    station = (lax.axis_index("expert") // 2).astype(jnp.int32).reshape(1)
    hbm = functools.partial(pltpu.with_memory_space_constraint, memory_space=pltpu.HBM)

    inputs = (
        tokens,
        norm_gain.reshape(1, width),
        expert_ids,
        route_score,
        expert_pair.reshape(1, stations),
    )
    payload, weights_first, *first = call(
        functools.partial(prepare_kernel, peers=peers, cap=cap, slots=slots_first, width=width),
        [SMEM] + [HBM] * 5,
        [((rows, width + table), BF16), ((rows, peers * slots_first), BF16)]
        + [((slots_first, width), BF16)] * peers,
        [pltpu.VMEM(x.shape, x.dtype) for x in inputs] + [pltpu.SemaphoreType.DMA((5,))],
    )(station, *[hbm(x) for x in inputs])

    column = [payload] + [swap(payload, k << up) for k in range(1, blocks)]
    first = [swap(first[j], (j + 1) << 1) for j in range(peers)]
    own, shares, weights, *chosen = call(
        functools.partial(
            select_kernel, blocks=blocks, peers=peers, cap=cap, slots=slots, width=width
        ),
        [SMEM] + [VMEM] * blocks,
        [((held, width), BF16), ((held, LANES), F32), ((held - rows, peers * slots), BF16)]
        + [((slots, width), BF16)] * peers,
    )(station, *column)

    arrived = [swap(chosen[j], (j + 1) << 1) for j in range(peers)]
    own = jnp.concatenate([own] + first, axis=0)
    other = swap(own, 1)
    owned = call(
        functools.partial(own_kernel, steps_in=steps_in, steps_out=steps_out),
        [VMEM, VMEM, HBM, HBM],
        [
            ((early, width), F32),
            ((early, width), BF16),
            ((width, 2 * half), BF16),
            ((half, width), BF16),
        ],
        [
            pltpu.VMEM((2 * early, width), BF16),
            pltpu.VMEM((2 * early, 2 * half), F32),
            pltpu.SemaphoreType.DMA((steps_in,)),
            pltpu.SemaphoreType.DMA,
        ],
        limit=10,
        flops=2400 * held * half * width,
    )
    keep, give, inward, outward = owned(own, other, hbm(w_in), hbm(w_out))
    got = swap(give, 1)

    pieces = arrived + [swap(block, 1) for block in arrived]
    results = call(
        functools.partial(peer_kernel, peers=peers, steps_out=steps_out),
        [VMEM] * (2 * peers + 2),
        [((slots, width), F32)] * peers + [((slots, width), BF16)] * peers,
        [pltpu.VMEM((2 * peers * slots, width), BF16)],
        limit=10,
    )(*pieces, inward, outward)
    back, back_first = [], []
    for j in range(peers):
        halves = swap(results[peers + j], 1)
        done = (results[j] + halves.astype(F32)).astype(BF16)
        back.append(swap(done, (j + 1) << 1))
        span = slice(held + j * slots_first, held + (j + 1) * slots_first)
        done = (keep[span] + got[span].astype(F32)).astype(BF16)
        back_first.append(swap(done, (j + 1) << 1))

    summed = call(
        functools.partial(combine_kernel, peers=peers),
        [VMEM] * (4 + peers),
        [((rows, width), F32)] + [((rows, width), BF16)] * (blocks - 1),
    )(shares, weights, keep, got, *back)
    returned = [swap(summed[k], k << up) for k in range(1, blocks)]
    (mixed,) = call(
        functools.partial(total_kernel, peers=peers),
        [VMEM] * (1 + peers + blocks),
        [((rows, width), BF16)],
    )(summed[0], weights_first, *back_first, *returned)
    return mixed


def shape_of(devices):
    bits = (devices // 2).bit_length() - 1
    low = bits // 2
    return 1 << (bits - low), 1 << low, low + 1


def solution(mesh):
    in_specs = (
        P(("groups", "expert"), None),
        P(),
        P(("groups", "expert"), None),
        P(("groups", "expert"), None),
        P("groups"),
        P(("groups", "expert"), None, None),
        P(("groups", "expert"), None, None),
    )
    out_specs = P(("groups", "expert"), None)
    return jax.shard_map(layer, mesh=mesh, in_specs=in_specs, out_specs=out_specs, check_vma=False)
```

```python
import functools

import jax
import jax.numpy as jnp
from jax import lax
from jax.experimental import pallas as pl
from jax.experimental.pallas import tpu as pltpu
from jax.sharding import PartitionSpec as P


LANES = 128
BF16 = jnp.bfloat16
F32 = jnp.float32
HBM = pl.BlockSpec(memory_space=pltpu.HBM)
VMEM = pl.BlockSpec(memory_space=pltpu.VMEM)
SMEM = pl.BlockSpec(memory_space=pltpu.SMEM)


def swap(block, mask):
    count = lax.axis_size("expert")
    return lax.ppermute(block, "expert", [(i, i ^ mask) for i in range(count)])


def picked_rows(placing, body):
    return lax.dot_general(placing, body, (((0,), (0,)), ((), ())), preferred_element_type=F32)


def slot_weights(table, station, peers, slots, cap, rows_each):
    rows = table.shape[0]
    row = lax.broadcasted_iota(jnp.int32, (rows, rows), 0)
    col = lax.broadcasted_iota(jnp.int32, (rows, rows), 1)
    earlier = (col < row) & (row // rows_each == col // rows_each)
    rank = jnp.dot(
        jnp.where(earlier, 1.0, 0.0).astype(BF16),
        jnp.where(table > 0.0, 1.0, 0.0).astype(BF16),
        preferred_element_type=F32,
    )
    base = lax.broadcasted_iota(jnp.int32, (rows, 1), 0) // rows_each * cap
    lane = lax.broadcasted_iota(jnp.int32, table.shape, 1)
    target = lax.broadcasted_iota(jnp.int32, (rows, peers * slots), 1)
    weights = jnp.zeros((rows, peers * slots), F32)
    for j in range(peers):
        pick = lane == (station ^ (j + 1))
        share = jnp.sum(jnp.where(pick, table, 0.0), axis=1, keepdims=True)
        ranked = jnp.sum(jnp.where(pick, rank, 0.0), axis=1, keepdims=True)
        slot = base + ranked.astype(jnp.int32) + j * slots
        weights = weights + jnp.where(target == slot, share, 0.0)
    return weights


def prepare_kernel(station, *refs, peers, cap, slots, width):
    sources = refs[:5]
    payload, weights = refs[5:7]
    chosen = refs[7 : 7 + peers]
    copied = refs[7 + peers : 12 + peers]
    sems = refs[-1]
    copies = [
        pltpu.make_async_copy(source, target, sems.at[n])
        for n, (source, target) in enumerate(zip(sources, copied))
    ]
    for copy in copies:
        copy.start()
    for copy in copies:
        copy.wait()
    tokens, gain, ids, score, pair = copied
    widened = tokens[...].astype(F32)
    meansq = jnp.mean(widened * widened, axis=-1, keepdims=True)
    normed = (widened * lax.rsqrt(meansq + 1e-06) * gain[...]).astype(BF16)
    payload[:, :width] = normed
    rows, top = ids.shape
    stations = pair.shape[1]
    shares = score[...] / jnp.sum(score[...], axis=-1, keepdims=True)
    labels = lax.broadcasted_iota(jnp.int32, (rows, stations), 1)
    named = jnp.zeros((rows, stations), F32)
    for k in range(top):
        named = named + jnp.where(ids[:, k : k + 1] == labels, shares[:, k : k + 1], 0.0)
    place = lax.broadcasted_iota(jnp.int32, (payload.shape[1] - width, stations), 0)
    moved = jnp.where(pair[...] == place, 1.0, 0.0).astype(BF16)
    table = lax.dot_general(
        named.astype(BF16), moved, (((1,), (1,)), ((), ())), preferred_element_type=F32
    )
    payload[:, width:] = table.astype(BF16)
    shared = slot_weights(table, station[0], peers, slots, cap, rows)
    weights[...] = shared.astype(BF16)
    placed = picked_rows(jnp.where(shared > 0.0, 1.0, 0.0).astype(BF16), normed)
    for j, ref in enumerate(chosen):
        ref[...] = placed[j * slots : (j + 1) * slots].astype(BF16)


def select_kernel(station, *refs, blocks, peers, cap, slots, width):
    payloads = refs[:blocks]
    own, shares, weights = refs[blocks : blocks + 3]
    chosen = refs[blocks + 3 :]
    rows = payloads[0].shape[0]
    gathered = jnp.concatenate([ref[...].astype(F32) for ref in payloads], axis=0)
    table = gathered[:, width:]
    body = gathered[:, :width].astype(BF16)
    own[...] = body
    lane = lax.broadcasted_iota(jnp.int32, table.shape, 1)
    share = jnp.sum(jnp.where(lane == station[0], table, 0.0), axis=1, keepdims=True)
    shares[...] = jnp.broadcast_to(share, shares.shape)
    shared = slot_weights(table[rows:], station[0], peers, slots, cap, rows)
    weights[...] = shared.astype(BF16)
    placed = picked_rows(jnp.where(shared > 0.0, 1.0, 0.0).astype(BF16), body[rows:])
    for j, ref in enumerate(chosen):
        ref[...] = placed[j * slots : (j + 1) * slots].astype(BF16)


def activate(projected):
    half = projected.shape[1] // 2
    gate = projected[:, :half]
    return (gate / (1.0 + jnp.exp(-gate)) * projected[:, half:]).astype(BF16)


def own_kernel(
    own, first, other, w_in, w_out, keep, keep_first, give_first, inward, outward, stacked, acc, in_sem, out_sem, *, steps_in, steps_out
):
    held, width = own.shape
    extra = first.shape[0]
    k_len = width // steps_in
    n_len = width // steps_out
    copies_in = [
        pltpu.make_async_copy(
            w_in.at[0, pl.ds(s * k_len, k_len)], inward.at[pl.ds(s * k_len, k_len)], in_sem.at[s]
        )
        for s in range(steps_in)
    ]
    copy_out = pltpu.make_async_copy(w_out.at[0], outward, out_sem)
    for copy in copies_in:
        copy.start()
    copy_out.start()
    stacked[:held] = own[...]
    stacked[held : held + extra] = first[...]
    stacked[held + extra :] = other[...]
    for s in range(steps_in):
        span = slice(s * k_len, (s + 1) * k_len)
        copies_in[s].wait()
        part = jnp.dot(stacked[:, span], inward[span], preferred_element_type=F32)
        if s == 0:
            acc[...] = part
        else:
            acc[...] += part
    hidden = activate(acc[...])
    copy_out.wait()
    for s in range(steps_out):
        cols = slice(s * n_len, (s + 1) * n_len)
        value = jnp.dot(hidden, outward[:, cols], preferred_element_type=F32)
        keep[:, cols] = value[:held]
        keep_first[:, cols] = value[held : held + extra]
        give_first[:, cols] = value[held + extra :].astype(BF16)


def peer_kernel(*refs, peers, steps_out):
    pieces = refs[: 2 * peers + 1]
    inward, outward = refs[2 * peers + 1 : 2 * peers + 3]
    results = refs[2 * peers + 3 : 4 * peers + 4]
    stacked = refs[-1]
    width = pieces[0].shape[1]
    ends = [0]
    for ref in pieces:
        ends.append(ends[-1] + ref.shape[0])
        stacked[ends[-2] : ends[-1]] = ref[...]
    hidden = activate(jnp.dot(stacked[...], inward[...], preferred_element_type=F32))
    n_len = width // steps_out
    for s in range(steps_out):
        cols = slice(s * n_len, (s + 1) * n_len)
        value = jnp.dot(hidden, outward[:, cols], preferred_element_type=F32)
        for p, ref in enumerate(results):
            ref[:, cols] = value[ends[p] : ends[p + 1]].astype(ref.dtype)


def combine_kernel(shares, weights, keep, got, *refs, peers):
    back = refs[:peers]
    blocks = refs[peers:]
    stacked = jnp.concatenate([ref[...] for ref in back], axis=0)
    mixed = jnp.dot(weights[...], stacked, preferred_element_type=F32)
    local = shares[:, :1] * (keep[...] + got[...].astype(F32))
    rows = blocks[0].shape[0]
    blocks[0][...] = local[:rows]
    for b, ref in enumerate(blocks[1:]):
        span = slice(b * rows, (b + 1) * rows)
        ref[...] = (mixed[span] + local[rows:][span]).astype(BF16)


def total_kernel(local, weights, *refs, peers):
    back = refs[:peers]
    stacked = jnp.concatenate([ref[...] for ref in back], axis=0)
    total = local[...] + jnp.dot(weights[...], stacked, preferred_element_type=F32)
    for ref in refs[peers:-1]:
        total = total + ref[...].astype(F32)
    refs[-1][...] = total.astype(BF16)


def call(kernel, ins, outs, scratch=(), limit=6, flops=0, moved=0):
    return pl.pallas_call(
        kernel,
        in_specs=list(ins),
        out_specs=[VMEM] * len(outs),
        out_shape=[jax.ShapeDtypeStruct(*out) for out in outs],
        scratch_shapes=list(scratch),
        cost_estimate=pl.CostEstimate(flops=flops, bytes_accessed=moved, transcendentals=0),
        compiler_params=pltpu.CompilerParams(vmem_limit_bytes=limit << 20),
    )


def layer(tokens, norm_gain, expert_ids, route_score, expert_pair, w_in, w_out):
    devices = lax.axis_size("expert")
    blocks, plane, up = shape_of(devices)
    peers = plane - 1
    stations = expert_pair.shape[0]
    rows, top = expert_ids.shape
    width = tokens.shape[1]
    half = w_out.shape[1]
    cap = min(rows, -(-rows * top // stations) + 1)
    slots_first = -(-cap // 8) * 8
    slots = -(-(blocks - 1) * cap // 8) * 8
    table = -(-stations // LANES) * LANES
    held = blocks * rows
    steps_in, steps_out = 8, 4
    station = (lax.axis_index("expert") // 2).astype(jnp.int32).reshape(1)
    hbm = functools.partial(pltpu.with_memory_space_constraint, memory_space=pltpu.HBM)

    inputs = (
        tokens,
        norm_gain.reshape(1, width),
        expert_ids,
        route_score,
        expert_pair.reshape(1, stations),
    )
    payload, weights_first, *first = call(
        functools.partial(prepare_kernel, peers=peers, cap=cap, slots=slots_first, width=width),
        [SMEM] + [HBM] * 5,
        [((rows, width + table), BF16), ((rows, peers * slots_first), BF16)]
        + [((slots_first, width), BF16)] * peers,
        [pltpu.VMEM(x.shape, x.dtype) for x in inputs] + [pltpu.SemaphoreType.DMA((5,))],
    )(station, *[hbm(x) for x in inputs])

    column = [payload] + [swap(payload, k << up) for k in range(1, blocks)]
    first = [swap(first[j], (j + 1) << 1) for j in range(peers)]
    own, shares, weights, *chosen = call(
        functools.partial(
            select_kernel, blocks=blocks, peers=peers, cap=cap, slots=slots, width=width
        ),
        [SMEM] + [VMEM] * blocks,
        [((held, width), BF16), ((held, LANES), F32), ((held - rows, peers * slots), BF16)]
        + [((slots, width), BF16)] * peers,
    )(station, *column)

    arrived = [swap(chosen[j], (j + 1) << 1) for j in range(peers)]
    other = swap(own, 1)
    first = jnp.concatenate(first, axis=0)
    other_first = swap(first, 1)
    extra = peers * slots_first
    total = held + 2 * extra
    owned = call(
        functools.partial(own_kernel, steps_in=steps_in, steps_out=steps_out),
        [VMEM] * 3 + [HBM] * 2,
        [
            ((held, width), F32),
            ((extra, width), F32),
            ((extra, width), BF16),
            ((width, 2 * half), BF16),
            ((half, width), BF16),
        ],
        [
            pltpu.VMEM((total, width), BF16),
            pltpu.VMEM((total, 2 * half), F32),
            pltpu.SemaphoreType.DMA((steps_in,)),
            pltpu.SemaphoreType.DMA,
        ],
        limit=10,
        flops=2400 * held * half * width,
    )
    keep, keep_first, give_first, inward, outward = owned(
        own, first, other_first, hbm(w_in), hbm(w_out)
    )
    got_first = swap(give_first, 1)

    swapped = [swap(block, 1) for block in arrived]
    peer_call = call(
        functools.partial(peer_kernel, peers=peers, steps_out=steps_out),
        [VMEM] * (2 * peers + 3),
        [((slots, width), F32)] * peers
        + [((slots, width), BF16)] * peers
        + [((held, width), BF16)],
        [pltpu.VMEM((2 * peers * slots + held, width), BF16)],
        limit=12,
    )
    results = peer_call(*arrived, *swapped, other, inward, outward)
    got = swap(results[-1], 1)
    back, back_first = [], []
    for j in range(peers):
        halves = swap(results[peers + j], 1)
        done = (results[j] + halves.astype(F32)).astype(BF16)
        back.append(swap(done, (j + 1) << 1))
        span = slice(j * slots_first, (j + 1) * slots_first)
        done = (keep_first[span] + got_first[span].astype(F32)).astype(BF16)
        back_first.append(swap(done, (j + 1) << 1))

    summed = call(
        functools.partial(combine_kernel, peers=peers),
        [VMEM] * (4 + peers),
        [((rows, width), F32)] + [((rows, width), BF16)] * (blocks - 1),
    )(shares, weights, keep, got, *back)
    returned = [swap(summed[k], k << up) for k in range(1, blocks)]
    (mixed,) = call(
        functools.partial(total_kernel, peers=peers),
        [VMEM] * (1 + peers + blocks),
        [((rows, width), BF16)],
    )(summed[0], weights_first, *back_first, *returned)
    return mixed


def shape_of(devices):
    bits = (devices // 2).bit_length() - 1
    low = bits // 2
    return 1 << (bits - low), 1 << low, low + 1


def solution(mesh):
    in_specs = (
        P(("groups", "expert"), None),
        P(),
        P(("groups", "expert"), None),
        P(("groups", "expert"), None),
        P("groups"),
        P(("groups", "expert"), None, None),
        P(("groups", "expert"), None, None),
    )
    out_specs = P(("groups", "expert"), None)
    return jax.shard_map(layer, mesh=mesh, in_specs=in_specs, out_specs=out_specs, check_vma=False)
```

```python
import functools

import jax
import jax.numpy as jnp
from jax import lax
from jax.experimental import pallas as pl
from jax.experimental.pallas import tpu as pltpu
from jax.sharding import PartitionSpec as P


LANES = 128
BF16 = jnp.bfloat16
F32 = jnp.float32
HBM = pl.BlockSpec(memory_space=pltpu.HBM)
VMEM = pl.BlockSpec(memory_space=pltpu.VMEM)
SMEM = pl.BlockSpec(memory_space=pltpu.SMEM)


def swap(block, mask):
    count = lax.axis_size("expert")
    return lax.ppermute(block, "expert", [(i, i ^ mask) for i in range(count)])


def picked_rows(placing, body):
    return lax.dot_general(placing, body, (((0,), (0,)), ((), ())), preferred_element_type=F32)


def slot_weights(table, station, peers, slots, cap, rows_each):
    rows = table.shape[0]
    row = lax.broadcasted_iota(jnp.int32, (rows, rows), 0)
    col = lax.broadcasted_iota(jnp.int32, (rows, rows), 1)
    earlier = (col < row) & (row // rows_each == col // rows_each)
    rank = jnp.dot(
        jnp.where(earlier, 1.0, 0.0).astype(BF16),
        jnp.where(table > 0.0, 1.0, 0.0).astype(BF16),
        preferred_element_type=F32,
    )
    base = lax.broadcasted_iota(jnp.int32, (rows, 1), 0) // rows_each * cap
    lane = lax.broadcasted_iota(jnp.int32, table.shape, 1)
    target = lax.broadcasted_iota(jnp.int32, (rows, peers * slots), 1)
    weights = jnp.zeros((rows, peers * slots), F32)
    for j in range(peers):
        pick = lane == (station ^ (j + 1))
        share = jnp.sum(jnp.where(pick, table, 0.0), axis=1, keepdims=True)
        ranked = jnp.sum(jnp.where(pick, rank, 0.0), axis=1, keepdims=True)
        slot = base + ranked.astype(jnp.int32) + j * slots
        weights = weights + jnp.where(target == slot, share, 0.0)
    return weights


def prepare_kernel(station, *refs, peers, cap, slots, width):
    sources = refs[:5]
    payload, weights = refs[5:7]
    chosen = refs[7 : 7 + peers]
    copied = refs[7 + peers : 12 + peers]
    sems = refs[-1]
    copies = [
        pltpu.make_async_copy(source, target, sems.at[n])
        for n, (source, target) in enumerate(zip(sources, copied))
    ]
    for copy in copies:
        copy.start()
    for copy in copies:
        copy.wait()
    tokens, gain, ids, score, pair = copied
    widened = tokens[...].astype(F32)
    meansq = jnp.mean(widened * widened, axis=-1, keepdims=True)
    normed = (widened * lax.rsqrt(meansq + 1e-06) * gain[...]).astype(BF16)
    payload[:, :width] = normed
    rows, top = ids.shape
    stations = pair.shape[1]
    shares = score[...] / jnp.sum(score[...], axis=-1, keepdims=True)
    labels = lax.broadcasted_iota(jnp.int32, (rows, stations), 1)
    named = jnp.zeros((rows, stations), F32)
    for k in range(top):
        named = named + jnp.where(ids[:, k : k + 1] == labels, shares[:, k : k + 1], 0.0)
    place = lax.broadcasted_iota(jnp.int32, (payload.shape[1] - width, stations), 0)
    moved = jnp.where(pair[...] == place, 1.0, 0.0).astype(BF16)
    table = lax.dot_general(
        named.astype(BF16), moved, (((1,), (1,)), ((), ())), preferred_element_type=F32
    )
    payload[:, width:] = table.astype(BF16)
    shared = slot_weights(table, station[0], peers, slots, cap, rows)
    weights[...] = shared.astype(BF16)
    placed = picked_rows(jnp.where(shared > 0.0, 1.0, 0.0).astype(BF16), normed)
    for j, ref in enumerate(chosen):
        ref[...] = placed[j * slots : (j + 1) * slots].astype(BF16)


def select_kernel(station, *refs, blocks, peers, cap, slots, width):
    payloads = refs[:blocks]
    own, shares, weights = refs[blocks : blocks + 3]
    chosen = refs[blocks + 3 :]
    rows = payloads[0].shape[0]
    gathered = jnp.concatenate([ref[...].astype(F32) for ref in payloads], axis=0)
    table = gathered[:, width:]
    body = gathered[:, :width].astype(BF16)
    own[...] = body
    lane = lax.broadcasted_iota(jnp.int32, table.shape, 1)
    share = jnp.sum(jnp.where(lane == station[0], table, 0.0), axis=1, keepdims=True)
    shares[...] = jnp.broadcast_to(share, shares.shape)
    shared = slot_weights(table[rows:], station[0], peers, slots, cap, rows)
    weights[...] = shared.astype(BF16)
    placed = picked_rows(jnp.where(shared > 0.0, 1.0, 0.0).astype(BF16), body[rows:])
    for j, ref in enumerate(chosen):
        ref[...] = placed[j * slots : (j + 1) * slots].astype(BF16)


def activate(projected):
    half = projected.shape[1] // 2
    gate = projected[:, :half]
    return (gate / (1.0 + jnp.exp(-gate)) * projected[:, half:]).astype(BF16)


def load_kernel(weights, loaded, sems):
    steps = sems.shape[0]
    size = loaded.shape[0] // steps
    copies = [
        pltpu.make_async_copy(
            weights.at[0, pl.ds(s * size, size)], loaded.at[pl.ds(s * size, size)], sems.at[s]
        )
        for s in range(steps)
    ]
    for copy in copies:
        copy.start()
    for copy in copies:
        copy.wait()


def expert_kernel(*refs, pieces, steps_out):
    inputs = refs[:pieces]
    inward, outward = refs[pieces : pieces + 2]
    results = refs[pieces + 2 : -1]
    stacked = refs[-1]
    width = inputs[0].shape[1]
    ends = [0]
    for ref in inputs:
        ends.append(ends[-1] + ref.shape[0])
        stacked[ends[-2] : ends[-1]] = ref[...]
    hidden = activate(jnp.dot(stacked[...], inward[...], preferred_element_type=F32))
    n_len = width // steps_out
    for s in range(steps_out):
        cols = slice(s * n_len, (s + 1) * n_len)
        value = jnp.dot(hidden, outward[:, cols], preferred_element_type=F32)
        for p, ref in enumerate(results):
            ref[:, cols] = value[ends[p] : ends[p + 1]].astype(ref.dtype)


def combine_kernel(shares, weights, keep, got, *refs, peers):
    back = refs[:peers]
    blocks = refs[peers:]
    stacked = jnp.concatenate([ref[...] for ref in back], axis=0)
    mixed = jnp.dot(weights[...], stacked, preferred_element_type=F32)
    held = shares.shape[0]
    local = shares[:, :1] * (keep[:held] + got[:held].astype(F32))
    rows = blocks[0].shape[0]
    blocks[0][...] = local[:rows]
    for b, ref in enumerate(blocks[1:]):
        span = slice(b * rows, (b + 1) * rows)
        ref[...] = (mixed[span] + local[rows:][span]).astype(BF16)


def total_kernel(local, weights, *refs, peers):
    back = refs[:peers]
    stacked = jnp.concatenate([ref[...] for ref in back], axis=0)
    total = local[...] + jnp.dot(weights[...], stacked, preferred_element_type=F32)
    for ref in refs[peers:-1]:
        total = total + ref[...].astype(F32)
    refs[-1][...] = total.astype(BF16)


def call(kernel, ins, outs, scratch=(), limit=6, flops=0, moved=0):
    return pl.pallas_call(
        kernel,
        in_specs=list(ins),
        out_specs=[VMEM] * len(outs),
        out_shape=[jax.ShapeDtypeStruct(*out) for out in outs],
        scratch_shapes=list(scratch),
        cost_estimate=pl.CostEstimate(flops=flops, bytes_accessed=moved, transcendentals=0),
        compiler_params=pltpu.CompilerParams(vmem_limit_bytes=limit << 20),
    )


def load(weights, steps=8):
    kernel = call(
        load_kernel, [HBM], [(weights.shape[1:], weights.dtype)], [pltpu.SemaphoreType.DMA((steps,))]
    )
    return kernel(weights)[0]


def layer(tokens, norm_gain, expert_ids, route_score, expert_pair, w_in, w_out):
    devices = lax.axis_size("expert")
    blocks, plane, up = shape_of(devices)
    peers = plane - 1
    stations = expert_pair.shape[0]
    rows, top = expert_ids.shape
    width = tokens.shape[1]
    cap = min(rows, -(-rows * top // stations) + 1)
    slots_first = -(-cap // 8) * 8
    slots = -(-(blocks - 1) * cap // 8) * 8
    table = -(-stations // LANES) * LANES
    held = blocks * rows
    early = held + peers * slots_first
    station = (lax.axis_index("expert") // 2).astype(jnp.int32).reshape(1)
    hbm = functools.partial(pltpu.with_memory_space_constraint, memory_space=pltpu.HBM)

    inputs = (
        tokens,
        norm_gain.reshape(1, width),
        expert_ids,
        route_score,
        expert_pair.reshape(1, stations),
    )
    payload, weights_first, *first = call(
        functools.partial(prepare_kernel, peers=peers, cap=cap, slots=slots_first, width=width),
        [SMEM] + [HBM] * 5,
        [((rows, width + table), BF16), ((rows, peers * slots_first), BF16)]
        + [((slots_first, width), BF16)] * peers,
        [pltpu.VMEM(x.shape, x.dtype) for x in inputs] + [pltpu.SemaphoreType.DMA((5,))],
    )(station, *[hbm(x) for x in inputs])

    inward = load(hbm(w_in))
    outward = load(hbm(w_out))
    column = [payload] + [swap(payload, k << up) for k in range(1, blocks)]
    first = [swap(first[j], (j + 1) << 1) for j in range(peers)]
    own, shares, weights, *chosen = call(
        functools.partial(
            select_kernel, blocks=blocks, peers=peers, cap=cap, slots=slots, width=width
        ),
        [SMEM] + [VMEM] * blocks,
        [((held, width), BF16), ((held, LANES), F32), ((held - rows, peers * slots), BF16)]
        + [((slots, width), BF16)] * peers,
    )(station, *column)

    arrived = [swap(chosen[j], (j + 1) << 1) for j in range(peers)]
    own = jnp.concatenate([own] + first, axis=0)
    other = swap(own, 1)
    swapped = [swap(block, 1) for block in arrived]
    pieces = arrived + swapped + [own, other]
    experts = call(
        functools.partial(expert_kernel, pieces=len(pieces), steps_out=4),
        [VMEM] * (len(pieces) + 2),
        [((slots, width), F32)] * peers
        + [((slots, width), BF16)] * peers
        + [((early, width), F32), ((early, width), BF16)],
        [pltpu.VMEM((2 * (peers * slots + early), width), BF16)],
        limit=16,
    )
    *results, keep, give = experts(*pieces, inward, outward)
    got = swap(give, 1)
    back, back_first = [], []
    for j in range(peers):
        halves = swap(results[peers + j], 1)
        done = (results[j] + halves.astype(F32)).astype(BF16)
        back.append(swap(done, (j + 1) << 1))
        span = slice(held + j * slots_first, held + (j + 1) * slots_first)
        done = (keep[span] + got[span].astype(F32)).astype(BF16)
        back_first.append(swap(done, (j + 1) << 1))

    combine = call(
        functools.partial(combine_kernel, peers=peers),
        [VMEM] * (4 + peers),
        [((rows, width), F32)] + [((rows, width), BF16)] * (blocks - 1),
    )
    summed = combine(shares, weights, keep, got, *back)
    returned = [swap(summed[k], k << up) for k in range(1, blocks)]
    (mixed,) = call(
        functools.partial(total_kernel, peers=peers),
        [VMEM] * (1 + peers + blocks),
        [((rows, width), BF16)],
    )(summed[0], weights_first, *back_first, *returned)
    return mixed


def shape_of(devices):
    bits = (devices // 2).bit_length() - 1
    low = bits // 2
    return 1 << (bits - low), 1 << low, low + 1


def solution(mesh):
    in_specs = (
        P(("groups", "expert"), None),
        P(),
        P(("groups", "expert"), None),
        P(("groups", "expert"), None),
        P("groups"),
        P(("groups", "expert"), None, None),
        P(("groups", "expert"), None, None),
    )
    out_specs = P(("groups", "expert"), None)
    return jax.shard_map(layer, mesh=mesh, in_specs=in_specs, out_specs=out_specs, check_vma=False)
```

```python
import functools

import jax
import jax.numpy as jnp
from jax import lax
from jax.experimental import pallas as pl
from jax.experimental.pallas import tpu as pltpu
from jax.sharding import PartitionSpec as P


LANES = 128
BF16 = jnp.bfloat16
F32 = jnp.float32
HBM = pl.BlockSpec(memory_space=pltpu.HBM)
VMEM = pl.BlockSpec(memory_space=pltpu.VMEM)
SMEM = pl.BlockSpec(memory_space=pltpu.SMEM)


def swap(block, mask):
    count = lax.axis_size("expert")
    return lax.ppermute(block, "expert", [(i, i ^ mask) for i in range(count)])


def picked_rows(placing, body):
    return lax.dot_general(placing, body, (((0,), (0,)), ((), ())), preferred_element_type=F32)


def slot_weights(table, station, peers, slots, cap, rows_each, first=0):
    rows = table.shape[0]
    row = lax.broadcasted_iota(jnp.int32, (rows, rows), 0)
    col = lax.broadcasted_iota(jnp.int32, (rows, rows), 1)
    earlier = (col < row) & (row // rows_each == col // rows_each)
    rank = jnp.dot(
        jnp.where(earlier, 1.0, 0.0).astype(BF16),
        jnp.where(table > 0.0, 1.0, 0.0).astype(BF16),
        preferred_element_type=F32,
    )
    block = lax.broadcasted_iota(jnp.int32, (rows, 1), 0) // rows_each
    base = jnp.where(block < first, block + rows // rows_each, block) * cap - first * cap
    lane = lax.broadcasted_iota(jnp.int32, table.shape, 1)
    target = lax.broadcasted_iota(jnp.int32, (rows, peers * slots), 1)
    weights = jnp.zeros((rows, peers * slots), F32)
    for j in range(peers):
        pick = lane == (station ^ (j + 1))
        share = jnp.sum(jnp.where(pick, table, 0.0), axis=1, keepdims=True)
        ranked = jnp.sum(jnp.where(pick, rank, 0.0), axis=1, keepdims=True)
        slot = base + ranked.astype(jnp.int32) + j * slots
        weights = weights + jnp.where(target == slot, share, 0.0)
    return weights


def prepare_kernel(station, *refs, peers, cap, slots, width):
    sources = refs[:5]
    heavy = refs[5]
    payload, loaded = refs[6:8]
    chosen = refs[8 : 8 + peers]
    copied = refs[8 + peers : 13 + peers]
    sems, heavy_sems = refs[-2:]
    copies = [
        pltpu.make_async_copy(source, target, sems.at[n])
        for n, (source, target) in enumerate(zip(sources, copied))
    ]
    for copy in copies:
        copy.start()
    weights = pieces_of(heavy, loaded, heavy_sems, 0)
    for copy in weights:
        copy.start()
    for copy in copies:
        copy.wait()
    tokens, gain, ids, score, pair = copied
    widened = tokens[...].astype(F32)
    meansq = jnp.mean(widened * widened, axis=-1, keepdims=True)
    normed = (widened * lax.rsqrt(meansq + 1e-06) * gain[...]).astype(BF16)
    payload[:, :width] = normed
    rows, top = ids.shape
    stations = pair.shape[1]
    shares = score[...] / jnp.sum(score[...], axis=-1, keepdims=True)
    labels = lax.broadcasted_iota(jnp.int32, (rows, stations), 1)
    named = jnp.zeros((rows, stations), F32)
    for k in range(top):
        named = named + jnp.where(ids[:, k : k + 1] == labels, shares[:, k : k + 1], 0.0)
    place = lax.broadcasted_iota(jnp.int32, (payload.shape[1] - width, stations), 0)
    moved = jnp.where(pair[...] == place, 1.0, 0.0).astype(BF16)
    table = lax.dot_general(
        named.astype(BF16), moved, (((1,), (1,)), ((), ())), preferred_element_type=F32
    )
    payload[:, width:] = table.astype(BF16)
    shared = slot_weights(table, station[0], peers, slots, cap, rows)
    placed = picked_rows(jnp.where(shared > 0.0, 1.0, 0.0).astype(BF16), normed)
    for j, ref in enumerate(chosen):
        ref[...] = placed[j * slots : (j + 1) * slots].astype(BF16)
    for copy in weights:
        copy.wait()


def select_kernel(station, *refs, blocks, peers, cap, slots, width):
    payloads = refs[:blocks]
    own, tables = refs[blocks : blocks + 2]
    chosen = refs[blocks + 2 :]
    rows = payloads[0].shape[0]
    gathered = jnp.concatenate([ref[...].astype(F32) for ref in payloads], axis=0)
    table = gathered[:, width:]
    body = gathered[:, :width].astype(BF16)
    own[...] = body
    tables[...] = table
    shared = slot_weights(table[rows:], station[0], peers, slots, cap, rows)
    placed = picked_rows(jnp.where(shared > 0.0, 1.0, 0.0).astype(BF16), body[rows:])
    for j, ref in enumerate(chosen):
        ref[...] = placed[j * slots : (j + 1) * slots].astype(BF16)


def weigh_kernel(station, tables, shares, weights, *, peers, cap, rows_each):
    table = tables[...]
    lane = lax.broadcasted_iota(jnp.int32, table.shape, 1)
    share = jnp.sum(jnp.where(lane == station[0], table, 0.0), axis=1, keepdims=True)
    shares[...] = jnp.broadcast_to(share, shares.shape)
    folds, _, lanes = weights.shape
    back = lanes // peers // folds
    for s in range(folds):
        shared = slot_weights(table, station[0], peers, folds * back, cap, rows_each, 1)
        if s:
            shared = jnp.concatenate(
                [jnp.zeros((table.shape[0], s * back), F32), shared[:, : lanes - s * back]], axis=1
            )
        weights[s] = shared.astype(BF16)


def activate(projected):
    half = projected.shape[1] // 2
    gate = projected[:, :half]
    return (gate / (1.0 + jnp.exp(-gate)) * projected[:, half:]).astype(BF16)


def pieces_of(weights, loaded, sems, start):
    steps = sems.shape[0]
    size = loaded.shape[0] // steps
    return [
        pltpu.make_async_copy(
            weights.at[0, pl.ds(start + s * size, size)],
            loaded.at[pl.ds(s * size, size)],
            sems.at[s],
        )
        for s in range(steps)
    ]


def load_kernel(*refs, starts):
    count = len(starts)
    copies = []
    for n, start in enumerate(starts):
        copies += pieces_of(refs[n], refs[count + n], refs[2 * count + n], start)
    for copy in copies:
        copy.start()
    for copy in copies:
        copy.wait()


def hidden_of(stacked, inward):
    total = None
    start = 0
    for ref in inward:
        end = start + ref.shape[0]
        part = jnp.dot(stacked[:, start:end], ref[...], preferred_element_type=F32)
        total = part if total is None else total + part
        start = end
    return activate(total)


def peer_kernel(*refs, peers, parts, held, counts, folds, steps):
    arrived, swapped = refs[:peers], refs[peers : 2 * peers]
    own, other = refs[2 * peers : 2 * peers + 2]
    inward = refs[2 * peers + 2 : 2 * peers + 2 + parts]
    outward = refs[2 * peers + 2 + parts]
    results = refs[2 * peers + 3 + parts : -1]
    stacked = refs[-1]
    width = own.shape[1]
    slots = arrived[0].shape[0]
    for p, ref in enumerate(arrived + swapped):
        stacked[p * slots : (p + 1) * slots] = ref[...]
    base = 2 * peers * slots
    extra = own.shape[0] - held
    stacked[base : base + extra] = own[held:]
    stacked[base + extra :] = other[held:]
    hidden = hidden_of(stacked, inward)
    first = extra // peers
    later, early = counts
    n_len = width // folds // steps
    for c in range(steps):
        values = []
        for f in range(folds):
            start = f * (width // folds) + c * n_len
            values.append(
                jnp.dot(hidden, outward[:, start : start + n_len], preferred_element_type=F32)
            )
        for p, ref in enumerate(results):
            rows = []
            for value in values:
                rows.append(value[p * slots : p * slots + later])
                rows.append(value[base + p * first : base + p * first + early])
            ref[:, c * n_len : (c + 1) * n_len] = jnp.concatenate(rows, axis=0).astype(ref.dtype)


def own_kernel(*refs, parts, steps):
    own, other = refs[:2]
    inward, outward = refs[2 : 2 + parts], refs[2 + parts]
    keep, give = refs[3 + parts : 5 + parts]
    stacked = refs[-1]
    held, width = keep.shape
    stacked[:held] = own[:held]
    stacked[held:] = other[:held]
    hidden = hidden_of(stacked, inward)
    n_len = width // steps
    for c in range(steps):
        cols = slice(c * n_len, (c + 1) * n_len)
        value = jnp.dot(hidden, outward[:, cols], preferred_element_type=F32)
        keep[:, cols] = value[:held]
        give[:, cols] = value[held:].astype(BF16)


def combine_kernel(shares, weights, keep, got, *refs, peers):
    back = refs[:peers]
    blocks = refs[peers:]
    stacked = jnp.concatenate([ref[...] for ref in back], axis=0)
    folds = weights.shape[0]
    rows = blocks[0].shape[0]
    for f in range(folds):
        cols = slice(f * stacked.shape[1], (f + 1) * stacked.shape[1])
        mixed = jnp.dot(weights[f], stacked, preferred_element_type=F32)
        mixed = mixed + shares[:, :1] * (keep[:, cols] + got[:, cols].astype(F32))
        for b, ref in enumerate(blocks):
            ref[:, cols] = mixed[b * rows : (b + 1) * rows].astype(ref.dtype)


def total_kernel(local, *refs):
    total = local[...]
    for ref in refs[:-1]:
        total = total + ref[...].astype(F32)
    refs[-1][...] = total.astype(BF16)


def call(kernel, ins, outs, scratch=(), limit=6, flops=0, moved=0):
    return pl.pallas_call(
        kernel,
        in_specs=list(ins),
        out_specs=[VMEM] * len(outs),
        out_shape=[jax.ShapeDtypeStruct(*out) for out in outs],
        scratch_shapes=list(scratch),
        cost_estimate=pl.CostEstimate(flops=flops, bytes_accessed=moved, transcendentals=0),
        compiler_params=pltpu.CompilerParams(vmem_limit_bytes=limit << 20),
    )


def load(*wanted):
    kernel = call(
        functools.partial(load_kernel, starts=[start for _, start, _, _ in wanted]),
        [HBM] * len(wanted),
        [((size, weights.shape[2]), weights.dtype) for weights, _, size, _ in wanted],
        [pltpu.SemaphoreType.DMA((steps,)) for _, _, _, steps in wanted],
    )
    return kernel(*[weights for weights, _, _, _ in wanted])


def layer(tokens, norm_gain, expert_ids, route_score, expert_pair, w_in, w_out):
    devices = lax.axis_size("expert")
    blocks, plane, up = shape_of(devices)
    peers = plane - 1
    stations = expert_pair.shape[0]
    rows, top = expert_ids.shape
    width = tokens.shape[1]
    half = w_out.shape[1]
    cap = min(rows, -(-rows * top // stations) + 1)
    slots_first = -(-cap // 8) * 8
    slots = -(-(blocks - 1) * cap // 8) * 8
    count = blocks * cap
    folds = next(f for f in (1, 2, 4, 8) if f * count % 8 == 0)
    packed = (folds * count, width // folds)
    table = -(-stations // LANES) * LANES
    held = blocks * rows
    station = (lax.axis_index("expert") // 2).astype(jnp.int32).reshape(1)
    hbm = functools.partial(pltpu.with_memory_space_constraint, memory_space=pltpu.HBM)
    w_in, w_out = hbm(w_in), hbm(w_out)
    cuts = (width // 4, width * 3 // 8, width * 3 // 8)

    inputs = (
        tokens,
        norm_gain.reshape(1, width),
        expert_ids,
        route_score,
        expert_pair.reshape(1, stations),
    )
    payload, inward0, *first = call(
        functools.partial(prepare_kernel, peers=peers, cap=cap, slots=slots_first, width=width),
        [SMEM] + [HBM] * 6,
        [((rows, width + table), BF16), ((cuts[0], 2 * half), BF16)]
        + [((slots_first, width), BF16)] * peers,
        [pltpu.VMEM(x.shape, x.dtype) for x in inputs]
        + [pltpu.SemaphoreType.DMA((5,)), pltpu.SemaphoreType.DMA((4,))],
    )(station, *[hbm(x) for x in inputs], w_in)
    (inward1,) = load((w_in, cuts[0], cuts[1], 6))
    inward2, outward = load((w_in, cuts[0] + cuts[1], cuts[2], 6), (w_out, 0, half, 6))
    inward = [inward0, inward1, inward2]

    column = [payload] + [swap(payload, k << up) for k in range(1, blocks)]
    first = [swap(first[j], (j + 1) << 1) for j in range(peers)]
    own, tables, *chosen = call(
        functools.partial(
            select_kernel, blocks=blocks, peers=peers, cap=cap, slots=slots, width=width
        ),
        [SMEM] + [VMEM] * blocks,
        [((held, width), BF16), ((held, table), F32)]
        + [((slots, width), BF16)] * peers,
    )(station, *column)

    arrived = [swap(chosen[j], (j + 1) << 1) for j in range(peers)]
    own = jnp.concatenate([own] + first, axis=0)
    other = swap(own, 1)
    swapped = [swap(block, 1) for block in arrived]
    parts = len(inward)
    peer_call = call(
        functools.partial(
            peer_kernel,
            peers=peers,
            parts=parts,
            held=held,
            counts=((blocks - 1) * cap, cap),
            folds=folds,
            steps=2,
        ),
        [VMEM] * (2 * peers + 3 + parts),
        [(packed, F32)] * peers + [(packed, BF16)] * peers,
        [pltpu.VMEM((2 * peers * (slots + slots_first), width), BF16)],
        limit=16,
    )
    results = peer_call(*arrived, *swapped, own, other, *inward, outward)
    back = []
    for j in range(peers):
        halves = swap(results[peers + j], 1)
        done = (results[j] + halves.astype(F32)).astype(BF16)
        back.append(swap(done, (j + 1) << 1))
    own_call = call(
        functools.partial(own_kernel, parts=parts, steps=4),
        [VMEM] * (3 + parts),
        [((held, width), F32), ((held, width), BF16)],
        [pltpu.VMEM((2 * held, width), BF16)],
        limit=12,
    )
    keep, give = own_call(own, other, *inward, outward)
    got = swap(give, 1)
    weigh = call(
        functools.partial(weigh_kernel, peers=peers, cap=cap, rows_each=rows),
        [SMEM, VMEM],
        [((held, LANES), F32), ((folds, held, peers * packed[0]), BF16)],
    )
    shares, weights = weigh(station, tables)

    combine = call(
        functools.partial(combine_kernel, peers=peers),
        [VMEM] * (4 + peers),
        [((rows, width), F32)] + [((rows, width), BF16)] * (blocks - 1),
    )
    summed = combine(shares, weights, keep, got, *back)
    returned = [swap(summed[k], k << up) for k in range(1, blocks)]
    (mixed,) = call(total_kernel, [VMEM] * blocks, [((rows, width), BF16)])(summed[0], *returned)
    return mixed


def shape_of(devices):
    bits = (devices // 2).bit_length() - 1
    low = bits // 2
    return 1 << (bits - low), 1 << low, low + 1


def solution(mesh):
    in_specs = (
        P(("groups", "expert"), None),
        P(),
        P(("groups", "expert"), None),
        P(("groups", "expert"), None),
        P("groups"),
        P(("groups", "expert"), None, None),
        P(("groups", "expert"), None, None),
    )
    out_specs = P(("groups", "expert"), None)
    return jax.shard_map(layer, mesh=mesh, in_specs=in_specs, out_specs=out_specs, check_vma=False)
```

```python
import functools

import jax
import jax.numpy as jnp
from jax import lax
from jax.experimental import pallas as pl
from jax.experimental.pallas import tpu as pltpu
from jax.sharding import PartitionSpec as P


LANES = 128
BF16 = jnp.bfloat16
F32 = jnp.float32
HBM = pl.BlockSpec(memory_space=pltpu.HBM)
VMEM = pl.BlockSpec(memory_space=pltpu.VMEM)
SMEM = pl.BlockSpec(memory_space=pltpu.SMEM)


def swap(block, mask):
    count = lax.axis_size("expert")
    return lax.ppermute(block, "expert", [(i, i ^ mask) for i in range(count)])


def picked_rows(placing, body):
    return lax.dot_general(placing, body, (((0,), (0,)), ((), ())), preferred_element_type=F32)


def slot_weights(table, station, peers, slots, cap, rows_each):
    rows = table.shape[0]
    row = lax.broadcasted_iota(jnp.int32, (rows, rows), 0)
    col = lax.broadcasted_iota(jnp.int32, (rows, rows), 1)
    earlier = (col < row) & (row // rows_each == col // rows_each)
    rank = jnp.dot(
        jnp.where(earlier, 1.0, 0.0).astype(BF16),
        jnp.where(table > 0.0, 1.0, 0.0).astype(BF16),
        preferred_element_type=F32,
    )
    base = lax.broadcasted_iota(jnp.int32, (rows, 1), 0) // rows_each * cap
    lane = lax.broadcasted_iota(jnp.int32, table.shape, 1)
    target = lax.broadcasted_iota(jnp.int32, (rows, peers * slots), 1)
    weights = jnp.zeros((rows, peers * slots), F32)
    for j in range(peers):
        pick = lane == (station ^ (j + 1))
        share = jnp.sum(jnp.where(pick, table, 0.0), axis=1, keepdims=True)
        ranked = jnp.sum(jnp.where(pick, rank, 0.0), axis=1, keepdims=True)
        slot = base + ranked.astype(jnp.int32) + j * slots
        weights = weights + jnp.where(target == slot, share, 0.0)
    return weights


def prepare_kernel(station, *refs, peers, cap, slots, width):
    sources = refs[:5]
    heavy = refs[5]
    payload, loaded = refs[6:8]
    chosen = refs[8 : 8 + peers]
    copied = refs[8 + peers : 13 + peers]
    sems, heavy_sems = refs[-2:]
    copies = [
        pltpu.make_async_copy(source, target, sems.at[n])
        for n, (source, target) in enumerate(zip(sources, copied))
    ]
    for copy in copies:
        copy.start()
    weights = pieces_of(heavy, loaded, heavy_sems, 0)
    for copy in weights:
        copy.start()
    for copy in copies:
        copy.wait()
    tokens, gain, ids, score, pair = copied
    widened = tokens[...].astype(F32)
    meansq = jnp.mean(widened * widened, axis=-1, keepdims=True)
    normed = (widened * lax.rsqrt(meansq + 1e-06) * gain[...]).astype(BF16)
    payload[:, :width] = normed
    rows, top = ids.shape
    stations = pair.shape[1]
    shares = score[...] / jnp.sum(score[...], axis=-1, keepdims=True)
    labels = lax.broadcasted_iota(jnp.int32, (rows, stations), 1)
    named = jnp.zeros((rows, stations), F32)
    for k in range(top):
        named = named + jnp.where(ids[:, k : k + 1] == labels, shares[:, k : k + 1], 0.0)
    place = lax.broadcasted_iota(jnp.int32, (payload.shape[1] - width, stations), 0)
    moved = jnp.where(pair[...] == place, 1.0, 0.0).astype(BF16)
    table = lax.dot_general(
        named.astype(BF16), moved, (((1,), (1,)), ((), ())), preferred_element_type=F32
    )
    payload[:, width:] = table.astype(BF16)
    shared = slot_weights(table, station[0], peers, slots, cap, rows)
    placed = picked_rows(jnp.where(shared > 0.0, 1.0, 0.0).astype(BF16), normed)
    for j, ref in enumerate(chosen):
        ref[...] = placed[j * slots : (j + 1) * slots].astype(BF16)
    for copy in weights:
        copy.wait()


def select_kernel(station, *refs, blocks, peers, cap, slots, width):
    payloads = refs[:blocks]
    own, tables = refs[blocks : blocks + 2]
    chosen = refs[blocks + 2 :]
    rows = payloads[0].shape[0]
    gathered = jnp.concatenate([ref[...].astype(F32) for ref in payloads], axis=0)
    table = gathered[:, width:]
    body = gathered[:, :width].astype(BF16)
    own[...] = body
    tables[...] = table
    shared = slot_weights(table[rows:], station[0], peers, slots, cap, rows)
    placed = picked_rows(jnp.where(shared > 0.0, 1.0, 0.0).astype(BF16), body[rows:])
    for j, ref in enumerate(chosen):
        ref[...] = placed[j * slots : (j + 1) * slots].astype(BF16)


def weigh_kernel(station, tables, shares, *outs, peers, cap, rows_each):
    table = tables[...]
    lane = lax.broadcasted_iota(jnp.int32, table.shape, 1)
    share = jnp.sum(jnp.where(lane == station[0], table, 0.0), axis=1, keepdims=True)
    shares[...] = jnp.broadcast_to(share, shares.shape)
    for h, weights in enumerate(outs):
        folds, rows, lanes = weights.shape
        back = lanes // peers // folds
        part = table[h * rows : (h + 1) * rows]
        shared = slot_weights(part, station[0], peers, folds * back, cap, rows_each)
        weights[0] = shared.astype(BF16)
        for f in range(1, folds):
            shared = jnp.concatenate(
                [jnp.zeros((rows, back), F32), shared[:, : lanes - back]], axis=1
            )
            weights[f] = shared.astype(BF16)


def activate(projected):
    half = projected.shape[1] // 2
    gate = projected[:, :half]
    return (gate / (1.0 + jnp.exp(-gate)) * projected[:, half:]).astype(BF16)


def pieces_of(weights, loaded, sems, start):
    steps = sems.shape[0]
    size = loaded.shape[0] // steps
    return [
        pltpu.make_async_copy(
            weights.at[0, pl.ds(start + s * size, size)],
            loaded.at[pl.ds(s * size, size)],
            sems.at[s],
        )
        for s in range(steps)
    ]


def load_kernel(*refs, starts):
    count = len(starts)
    copies = []
    for n, start in enumerate(starts):
        copies += pieces_of(refs[n], refs[count + n], refs[2 * count + n], start)
    for copy in copies:
        copy.start()
    for copy in copies:
        copy.wait()


def hidden_of(stacked, inward):
    total = None
    start = 0
    for ref in inward:
        end = start + ref.shape[0]
        part = jnp.dot(stacked[:, start:end], ref[...], preferred_element_type=F32)
        total = part if total is None else total + part
        start = end
    return activate(total)


def expert_kernel(*refs, peers, parts, held, cap, near, far, folds, steps):
    arrived, swapped = refs[:peers], refs[peers : 2 * peers]
    own, other = refs[2 * peers : 2 * peers + 2]
    inward = refs[2 * peers + 2 : 2 * peers + 2 + parts]
    outward = refs[2 * peers + 2 + parts]
    results = refs[2 * peers + 3 + parts : -1]
    keep_far, give_far = results[:peers], results[peers : 2 * peers]
    keep_near, give_near, keep, give = results[2 * peers :]
    stacked = refs[-1]
    width = own.shape[1]
    slots = arrived[0].shape[0]
    pieces = arrived + swapped
    for p, ref in enumerate(pieces):
        stacked[p * slots : (p + 1) * slots] = ref[...]
    base = len(pieces) * slots
    early = own.shape[0]
    stacked[base : base + early] = own[...]
    stacked[base + early :] = other[...]
    hidden = hidden_of(stacked, inward)
    slots_first = (early - held) // peers
    n_len = width // folds // steps
    tall = folds * far * cap
    for c in range(steps):
        cols = slice(c * n_len, (c + 1) * n_len)
        values = []
        for f in range(folds):
            start = f * (width // folds) + c * n_len
            wide = slice(start, start + n_len)
            value = jnp.dot(hidden, outward[:, wide], preferred_element_type=F32)
            keep[:, wide] = value[base : base + held]
            give[:, wide] = value[base + early : base + early + held].astype(BF16)
            values.append(value)
        for p in range(2 * peers):
            side, j = divmod(p, peers)
            first = base + side * early + held + j * slots_first
            distant, close = [], []
            for value in values:
                start = p * slots + (near - 1) * cap
                distant.append(value[start : start + far * cap])
                close.append(value[first : first + cap])
                close.append(value[p * slots : start])
            ref = (give_far if side else keep_far)[j]
            ref[:, cols] = jnp.concatenate(distant, axis=0).astype(ref.dtype)
            ref = give_near if side else keep_near
            ref[j * tall : (j + 1) * tall, cols] = jnp.concatenate(close, axis=0).astype(ref.dtype)


def combine_kernel(shares, weights, keep, got, *refs, peers, start):
    back = refs[:peers]
    blocks = refs[peers:]
    stacked = jnp.concatenate([ref[...] for ref in back], axis=0)
    folds, size, _ = weights.shape
    span = slice(start, start + size)
    rows = blocks[0].shape[0]
    for f in range(folds):
        cols = slice(f * stacked.shape[1], (f + 1) * stacked.shape[1])
        mixed = jnp.dot(weights[f], stacked, preferred_element_type=F32)
        mixed = mixed + shares[span, :1] * (keep[span, cols] + got[span, cols].astype(F32))
        for b, ref in enumerate(blocks):
            ref[:, cols] = mixed[b * rows : (b + 1) * rows].astype(ref.dtype)


def total_kernel(local, *refs):
    total = local[...]
    for ref in refs[:-1]:
        total = total + ref[...].astype(F32)
    refs[-1][...] = total.astype(BF16)


def call(kernel, ins, outs, scratch=(), limit=6, flops=0, moved=0):
    return pl.pallas_call(
        kernel,
        in_specs=list(ins),
        out_specs=[VMEM] * len(outs),
        out_shape=[jax.ShapeDtypeStruct(*out) for out in outs],
        scratch_shapes=list(scratch),
        cost_estimate=pl.CostEstimate(flops=flops, bytes_accessed=moved, transcendentals=0),
        compiler_params=pltpu.CompilerParams(vmem_limit_bytes=limit << 20),
    )


def load(*wanted):
    kernel = call(
        functools.partial(load_kernel, starts=[start for _, start, _, _ in wanted]),
        [HBM] * len(wanted),
        [((size, weights.shape[2]), weights.dtype) for weights, _, size, _ in wanted],
        [pltpu.SemaphoreType.DMA((steps,)) for _, _, _, steps in wanted],
    )
    return kernel(*[weights for weights, _, _, _ in wanted])


def layer(tokens, norm_gain, expert_ids, route_score, expert_pair, w_in, w_out):
    devices = lax.axis_size("expert")
    blocks, plane, up = shape_of(devices)
    peers = plane - 1
    stations = expert_pair.shape[0]
    rows, top = expert_ids.shape
    width = tokens.shape[1]
    half = w_out.shape[1]
    cap = min(rows, -(-rows * top // stations) + 1)
    slots_first = -(-cap // 8) * 8
    slots = -(-(blocks - 1) * cap // 8) * 8
    near = blocks // 2
    far = blocks - near
    folds = next(f for f in (1, 2, 4, 8) if f * far * cap % 8 == 0)
    packed = (folds * far * cap, width // folds)
    table = -(-stations // LANES) * LANES
    held = blocks * rows
    early = held + peers * slots_first
    station = (lax.axis_index("expert") // 2).astype(jnp.int32).reshape(1)
    hbm = functools.partial(pltpu.with_memory_space_constraint, memory_space=pltpu.HBM)
    w_in, w_out = hbm(w_in), hbm(w_out)
    cuts = (width // 8, width * 3 // 8, width // 2)

    inputs = (
        tokens,
        norm_gain.reshape(1, width),
        expert_ids,
        route_score,
        expert_pair.reshape(1, stations),
    )
    payload, inward0, *first = call(
        functools.partial(prepare_kernel, peers=peers, cap=cap, slots=slots_first, width=width),
        [SMEM] + [HBM] * 6,
        [((rows, width + table), BF16), ((cuts[0], 2 * half), BF16)]
        + [((slots_first, width), BF16)] * peers,
        [pltpu.VMEM(x.shape, x.dtype) for x in inputs]
        + [pltpu.SemaphoreType.DMA((5,)), pltpu.SemaphoreType.DMA((4,))],
    )(station, *[hbm(x) for x in inputs], w_in)
    (inward1,) = load((w_in, cuts[0], cuts[1], 6))
    inward2, outward = load((w_in, cuts[0] + cuts[1], cuts[2], 8), (w_out, 0, half, 6))
    inward = [inward0, inward1, inward2]

    column = [payload] + [swap(payload, k << up) for k in range(1, blocks)]
    first = [swap(first[j], (j + 1) << 1) for j in range(peers)]
    own, tables, *chosen = call(
        functools.partial(
            select_kernel, blocks=blocks, peers=peers, cap=cap, slots=slots, width=width
        ),
        [SMEM] + [VMEM] * blocks,
        [((held, width), BF16), ((held, table), F32)]
        + [((slots, width), BF16)] * peers,
    )(station, *column)

    arrived = [swap(chosen[j], (j + 1) << 1) for j in range(peers)]
    own = jnp.concatenate([own] + first, axis=0)
    other = swap(own, 1)
    swapped = [swap(block, 1) for block in arrived]
    parts = len(inward)
    tall = packed[0]
    expert_call = call(
        functools.partial(
            expert_kernel,
            peers=peers,
            parts=parts,
            held=held,
            cap=cap,
            near=near,
            far=far,
            folds=folds,
            steps=1,
        ),
        [VMEM] * (2 * peers + 3 + parts),
        [(packed, F32)] * peers
        + [(packed, BF16)] * peers
        + [((peers * tall, packed[1]), kind) for kind in (F32, BF16)]
        + [((held, width), kind) for kind in (F32, BF16)],
        [pltpu.VMEM((2 * (peers * slots + early), width), BF16)],
        limit=20,
    )
    results = expert_call(*arrived, *swapped, own, other, *inward, outward)
    keep_near, give_near, keep, give = results[2 * peers :]
    back_far = []
    for j in range(peers):
        halves = swap(results[peers + j], 1)
        done = (results[j] + halves.astype(F32)).astype(BF16)
        back_far.append(swap(done, (j + 1) << 1))
    got_near = swap(give_near, 1)
    back_near = []
    for j in range(peers):
        span = slice(j * tall, (j + 1) * tall)
        done = (keep_near[span] + got_near[span].astype(F32)).astype(BF16)
        back_near.append(swap(done, (j + 1) << 1))
    got = swap(give, 1)
    weigh = call(
        functools.partial(weigh_kernel, peers=peers, cap=cap, rows_each=rows),
        [SMEM, VMEM],
        [((held, LANES), F32)] + [((folds, far * rows, peers * tall), BF16)] * 2,
    )
    shares, weights_near, weights_far = weigh(station, tables)

    def combine(start, weights, back, kinds):
        kernel = call(
            functools.partial(combine_kernel, peers=peers, start=start),
            [VMEM] * (4 + peers),
            [((rows, width), kind) for kind in kinds],
        )
        return kernel(shares, weights, keep, got, *back)

    summed_far = combine(near * rows, weights_far, back_far, [BF16] * far)
    summed_near = combine(0, weights_near, back_near, [F32] + [BF16] * (near - 1))
    summed = list(summed_near) + list(summed_far)
    returned = [swap(summed[k], k << up) for k in range(1, blocks)]
    (mixed,) = call(total_kernel, [VMEM] * blocks, [((rows, width), BF16)])(summed[0], *returned)
    return mixed


def shape_of(devices):
    bits = (devices // 2).bit_length() - 1
    low = bits // 2
    return 1 << (bits - low), 1 << low, low + 1


def solution(mesh):
    in_specs = (
        P(("groups", "expert"), None),
        P(),
        P(("groups", "expert"), None),
        P(("groups", "expert"), None),
        P("groups"),
        P(("groups", "expert"), None, None),
        P(("groups", "expert"), None, None),
    )
    out_specs = P(("groups", "expert"), None)
    return jax.shard_map(layer, mesh=mesh, in_specs=in_specs, out_specs=out_specs, check_vma=False)
```

```python
import functools

import jax
import jax.numpy as jnp
from jax import lax
from jax.experimental import pallas as pl
from jax.experimental.pallas import tpu as pltpu
from jax.sharding import PartitionSpec as P


LANES = 128
BF16 = jnp.bfloat16
F32 = jnp.float32
HBM = pl.BlockSpec(memory_space=pltpu.HBM)
VMEM = pl.BlockSpec(memory_space=pltpu.VMEM)
SMEM = pl.BlockSpec(memory_space=pltpu.SMEM)


def swap(block, mask):
    count = lax.axis_size("expert")
    return lax.ppermute(block, "expert", [(i, i ^ mask) for i in range(count)])


def picked_rows(placing, body):
    return lax.dot_general(placing, body, (((0,), (0,)), ((), ())), preferred_element_type=F32)


def slot_weights(table, station, peers, slots, cap, rows_each):
    rows = table.shape[0]
    row = lax.broadcasted_iota(jnp.int32, (rows, rows), 0)
    col = lax.broadcasted_iota(jnp.int32, (rows, rows), 1)
    earlier = (col < row) & (row // rows_each == col // rows_each)
    rank = jnp.dot(
        jnp.where(earlier, 1.0, 0.0).astype(BF16),
        jnp.where(table > 0.0, 1.0, 0.0).astype(BF16),
        preferred_element_type=F32,
    )
    base = lax.broadcasted_iota(jnp.int32, (rows, 1), 0) // rows_each * cap
    lane = lax.broadcasted_iota(jnp.int32, table.shape, 1)
    target = lax.broadcasted_iota(jnp.int32, (rows, peers * slots), 1)
    weights = jnp.zeros((rows, peers * slots), F32)
    for j in range(peers):
        pick = lane == (station ^ (j + 1))
        share = jnp.sum(jnp.where(pick, table, 0.0), axis=1, keepdims=True)
        ranked = jnp.sum(jnp.where(pick, rank, 0.0), axis=1, keepdims=True)
        slot = base + ranked.astype(jnp.int32) + j * slots
        weights = weights + jnp.where(target == slot, share, 0.0)
    return weights


def prepare_kernel(station, *refs, peers, cap, slots, width):
    sources = refs[:5]
    heavy = refs[5]
    payload, loaded = refs[6:8]
    chosen = refs[8 : 8 + peers]
    copied = refs[8 + peers : 13 + peers]
    sems, heavy_sems = refs[-2:]
    copies = [
        pltpu.make_async_copy(source, target, sems.at[n])
        for n, (source, target) in enumerate(zip(sources, copied))
    ]
    for copy in copies:
        copy.start()
    weights = pieces_of(heavy, loaded, heavy_sems, 0)
    for copy in weights:
        copy.start()
    for copy in copies:
        copy.wait()
    tokens, gain, ids, score, pair = copied
    widened = tokens[...].astype(F32)
    meansq = jnp.mean(widened * widened, axis=-1, keepdims=True)
    normed = (widened * lax.rsqrt(meansq + 1e-06) * gain[...]).astype(BF16)
    payload[:, :width] = normed
    rows, top = ids.shape
    stations = pair.shape[1]
    shares = score[...] / jnp.sum(score[...], axis=-1, keepdims=True)
    labels = lax.broadcasted_iota(jnp.int32, (rows, stations), 1)
    named = jnp.zeros((rows, stations), F32)
    for k in range(top):
        named = named + jnp.where(ids[:, k : k + 1] == labels, shares[:, k : k + 1], 0.0)
    place = lax.broadcasted_iota(jnp.int32, (payload.shape[1] - width, stations), 0)
    moved = jnp.where(pair[...] == place, 1.0, 0.0).astype(BF16)
    table = lax.dot_general(
        named.astype(BF16), moved, (((1,), (1,)), ((), ())), preferred_element_type=F32
    )
    payload[:, width:] = table.astype(BF16)
    shared = slot_weights(table, station[0], peers, slots, cap, rows)
    placed = picked_rows(jnp.where(shared > 0.0, 1.0, 0.0).astype(BF16), normed)
    for j, ref in enumerate(chosen):
        ref[...] = placed[j * slots : (j + 1) * slots].astype(BF16)
    for copy in weights:
        copy.wait()


def select_kernel(station, *refs, blocks, peers, cap, slots, width):
    payloads = refs[:blocks]
    own, tables = refs[blocks : blocks + 2]
    chosen = refs[blocks + 2 :]
    rows = payloads[0].shape[0]
    gathered = jnp.concatenate([ref[...].astype(F32) for ref in payloads], axis=0)
    table = gathered[:, width:]
    body = gathered[:, :width].astype(BF16)
    own[...] = body
    tables[...] = table
    shared = slot_weights(table[rows:], station[0], peers, slots, cap, rows)
    placed = picked_rows(jnp.where(shared > 0.0, 1.0, 0.0).astype(BF16), body[rows:])
    for j, ref in enumerate(chosen):
        ref[...] = placed[j * slots : (j + 1) * slots].astype(BF16)


def weigh(station, tables, shares, *outs, peers, cap, rows_each):
    table = tables[...]
    lane = lax.broadcasted_iota(jnp.int32, table.shape, 1)
    share = jnp.sum(jnp.where(lane == station[0], table, 0.0), axis=1, keepdims=True)
    shares[...] = jnp.broadcast_to(share, shares.shape)
    for h, weights in enumerate(outs):
        folds, rows, lanes = weights.shape
        back = lanes // peers // folds
        part = table[h * rows : (h + 1) * rows]
        shared = slot_weights(part, station[0], peers, folds * back, cap, rows_each)
        weights[0] = shared.astype(BF16)
        for f in range(1, folds):
            shared = jnp.concatenate(
                [jnp.zeros((rows, back), F32), shared[:, : lanes - back]], axis=1
            )
            weights[f] = shared.astype(BF16)


def activate(projected):
    half = projected.shape[1] // 2
    gate = projected[:, :half]
    return (gate / (1.0 + jnp.exp(-gate)) * projected[:, half:]).astype(BF16)


def pieces_of(weights, loaded, sems, start):
    steps = sems.shape[0]
    size = loaded.shape[0] // steps
    return [
        pltpu.make_async_copy(
            weights.at[0, pl.ds(start + s * size, size)],
            loaded.at[pl.ds(s * size, size)],
            sems.at[s],
        )
        for s in range(steps)
    ]


def load_kernel(*refs, starts):
    count = len(starts)
    copies = []
    for n, start in enumerate(starts):
        copies += pieces_of(refs[n], refs[count + n], refs[2 * count + n], start)
    for copy in copies:
        copy.start()
    for copy in copies:
        copy.wait()


def load_and_weigh_kernel(station, tables, *refs, starts, **sizes):
    count = len(starts)
    copies = []
    for n, start in enumerate(starts):
        copies += pieces_of(refs[n], refs[count + n], refs[2 * count + 3 + n], start)
    for copy in copies:
        copy.start()
    weigh(station, tables, *refs[2 * count : 2 * count + 3], **sizes)
    for copy in copies:
        copy.wait()


def hidden_of(stacked, inward):
    total = None
    start = 0
    for ref in inward:
        end = start + ref.shape[0]
        part = jnp.dot(stacked[:, start:end], ref[...], preferred_element_type=F32)
        total = part if total is None else total + part
        start = end
    return activate(total)


def expert_kernel(*refs, peers, parts, held, cap, near, far, folds, steps):
    arrived, swapped = refs[:peers], refs[peers : 2 * peers]
    own, other = refs[2 * peers : 2 * peers + 2]
    inward = refs[2 * peers + 2 : 2 * peers + 2 + parts]
    outward = refs[2 * peers + 2 + parts]
    results = refs[2 * peers + 3 + parts : -1]
    keep_far, give_far = results[:peers], results[peers : 2 * peers]
    keep_near, give_near, keep, give = results[2 * peers :]
    stacked = refs[-1]
    width = own.shape[1]
    slots = arrived[0].shape[0]
    pieces = arrived + swapped
    for p, ref in enumerate(pieces):
        stacked[p * slots : (p + 1) * slots] = ref[...]
    base = len(pieces) * slots
    early = own.shape[0]
    stacked[base : base + early] = own[...]
    stacked[base + early :] = other[...]
    hidden = hidden_of(stacked, inward)
    slots_first = (early - held) // peers
    n_len = width // folds // steps
    tall = folds * far * cap
    for c in range(steps):
        cols = slice(c * n_len, (c + 1) * n_len)
        values = []
        for f in range(folds):
            start = f * (width // folds) + c * n_len
            wide = slice(start, start + n_len)
            value = jnp.dot(hidden, outward[:, wide], preferred_element_type=F32)
            keep[:, wide] = value[base : base + held]
            give[:, wide] = value[base + early : base + early + held].astype(BF16)
            values.append(value)
        for p in range(2 * peers):
            side, j = divmod(p, peers)
            first = base + side * early + held + j * slots_first
            distant, close = [], []
            for value in values:
                start = p * slots + (near - 1) * cap
                distant.append(value[start : start + far * cap])
                close.append(value[first : first + cap])
                close.append(value[p * slots : start])
            ref = (give_far if side else keep_far)[j]
            ref[:, cols] = jnp.concatenate(distant, axis=0).astype(ref.dtype)
            ref = give_near if side else keep_near
            ref[j * tall : (j + 1) * tall, cols] = jnp.concatenate(close, axis=0).astype(ref.dtype)


def combine_kernel(shares, weights, keep, got, *refs, peers, start):
    back = refs[:peers]
    blocks = refs[peers:]
    stacked = jnp.concatenate([ref[...] for ref in back], axis=0)
    folds, size, _ = weights.shape
    span = slice(start, start + size)
    rows = blocks[0].shape[0]
    for f in range(folds):
        cols = slice(f * stacked.shape[1], (f + 1) * stacked.shape[1])
        mixed = jnp.dot(weights[f], stacked, preferred_element_type=F32)
        mixed = mixed + shares[span, :1] * (keep[span, cols] + got[span, cols].astype(F32))
        for b, ref in enumerate(blocks):
            ref[:, cols] = mixed[b * rows : (b + 1) * rows].astype(ref.dtype)


def total_kernel(local, *refs):
    total = local[...]
    for ref in refs[:-1]:
        total = total + ref[...].astype(F32)
    refs[-1][...] = total.astype(BF16)


def call(kernel, ins, outs, scratch=(), limit=6, flops=0, moved=0):
    return pl.pallas_call(
        kernel,
        in_specs=list(ins),
        out_specs=[VMEM] * len(outs),
        out_shape=[jax.ShapeDtypeStruct(*out) for out in outs],
        scratch_shapes=list(scratch),
        cost_estimate=pl.CostEstimate(flops=flops, bytes_accessed=moved, transcendentals=0),
        compiler_params=pltpu.CompilerParams(vmem_limit_bytes=limit << 20),
    )


def layer(tokens, norm_gain, expert_ids, route_score, expert_pair, w_in, w_out):
    devices = lax.axis_size("expert")
    blocks, plane, up = shape_of(devices)
    peers = plane - 1
    stations = expert_pair.shape[0]
    rows, top = expert_ids.shape
    width = tokens.shape[1]
    half = w_out.shape[1]
    cap = min(rows, -(-rows * top // stations) + 1)
    slots_first = -(-cap // 8) * 8
    slots = -(-(blocks - 1) * cap // 8) * 8
    near = blocks // 2
    far = blocks - near
    folds = next(f for f in (1, 2, 4, 8) if f * far * cap % 8 == 0)
    packed = (folds * far * cap, width // folds)
    table = -(-stations // LANES) * LANES
    held = blocks * rows
    early = held + peers * slots_first
    station = (lax.axis_index("expert") // 2).astype(jnp.int32).reshape(1)
    hbm = functools.partial(pltpu.with_memory_space_constraint, memory_space=pltpu.HBM)
    w_in, w_out = hbm(w_in), hbm(w_out)
    cuts = (width // 8, width * 3 // 8, width // 2)

    inputs = (
        tokens,
        norm_gain.reshape(1, width),
        expert_ids,
        route_score,
        expert_pair.reshape(1, stations),
    )
    payload, inward0, *first = call(
        functools.partial(prepare_kernel, peers=peers, cap=cap, slots=slots_first, width=width),
        [SMEM] + [HBM] * 6,
        [((rows, width + table), BF16), ((cuts[0], 2 * half), BF16)]
        + [((slots_first, width), BF16)] * peers,
        [pltpu.VMEM(x.shape, x.dtype) for x in inputs]
        + [pltpu.SemaphoreType.DMA((5,)), pltpu.SemaphoreType.DMA((4,))],
    )(station, *[hbm(x) for x in inputs], w_in)
    middle = call(
        functools.partial(load_kernel, starts=[cuts[0]]),
        [HBM],
        [((cuts[1], 2 * half), BF16)],
        [pltpu.SemaphoreType.DMA((6,))],
    )
    (inward1,) = middle(w_in)

    column = [payload] + [swap(payload, k << up) for k in range(1, blocks)]
    first = [swap(first[j], (j + 1) << 1) for j in range(peers)]
    own, tables, *chosen = call(
        functools.partial(
            select_kernel, blocks=blocks, peers=peers, cap=cap, slots=slots, width=width
        ),
        [SMEM] + [VMEM] * blocks,
        [((held, width), BF16), ((held, table), F32)]
        + [((slots, width), BF16)] * peers,
    )(station, *column)

    tall = packed[0]
    last = call(
        functools.partial(
            load_and_weigh_kernel,
            starts=[cuts[0] + cuts[1], 0],
            peers=peers,
            cap=cap,
            rows_each=rows,
        ),
        [SMEM, VMEM, HBM, HBM],
        [((cuts[2], 2 * half), BF16), ((half, width), BF16), ((held, LANES), F32)]
        + [((folds, far * rows, peers * tall), BF16)] * 2,
        [pltpu.SemaphoreType.DMA((8,)), pltpu.SemaphoreType.DMA((6,))],
    )
    inward2, outward, shares, weights_near, weights_far = last(station, tables, w_in, w_out)
    inward = [inward0, inward1, inward2]
    arrived = [swap(chosen[j], (j + 1) << 1) for j in range(peers)]
    own = jnp.concatenate([own] + first, axis=0)
    other = swap(own, 1)
    swapped = [swap(block, 1) for block in arrived]
    parts = len(inward)
    expert_call = call(
        functools.partial(
            expert_kernel,
            peers=peers,
            parts=parts,
            held=held,
            cap=cap,
            near=near,
            far=far,
            folds=folds,
            steps=1,
        ),
        [VMEM] * (2 * peers + 3 + parts),
        [(packed, F32)] * peers
        + [(packed, BF16)] * peers
        + [((peers * tall, packed[1]), kind) for kind in (F32, BF16)]
        + [((held, width), kind) for kind in (F32, BF16)],
        [pltpu.VMEM((2 * (peers * slots + early), width), BF16)],
        limit=20,
    )
    results = expert_call(*arrived, *swapped, own, other, *inward, outward)
    keep_near, give_near, keep, give = results[2 * peers :]
    back_far = []
    for j in range(peers):
        halves = swap(results[peers + j], 1)
        done = (results[j] + halves.astype(F32)).astype(BF16)
        back_far.append(swap(done, (j + 1) << 1))
    got_near = swap(give_near, 1)
    back_near = []
    for j in range(peers):
        span = slice(j * tall, (j + 1) * tall)
        done = (keep_near[span] + got_near[span].astype(F32)).astype(BF16)
        back_near.append(swap(done, (j + 1) << 1))
    got = swap(give, 1)
    def combine(start, weights, back, kinds):
        kernel = call(
            functools.partial(combine_kernel, peers=peers, start=start),
            [VMEM] * (4 + peers),
            [((rows, width), kind) for kind in kinds],
        )
        return kernel(shares, weights, keep, got, *back)

    summed_far = combine(near * rows, weights_far, back_far, [BF16] * far)
    summed_near = combine(0, weights_near, back_near, [F32] + [BF16] * (near - 1))
    summed = list(summed_near) + list(summed_far)
    returned = [swap(summed[k], k << up) for k in range(1, blocks)]
    (mixed,) = call(total_kernel, [VMEM] * blocks, [((rows, width), BF16)])(summed[0], *returned)
    return mixed


def shape_of(devices):
    bits = (devices // 2).bit_length() - 1
    low = bits // 2
    return 1 << (bits - low), 1 << low, low + 1


def solution(mesh):
    in_specs = (
        P(("groups", "expert"), None),
        P(),
        P(("groups", "expert"), None),
        P(("groups", "expert"), None),
        P("groups"),
        P(("groups", "expert"), None, None),
        P(("groups", "expert"), None, None),
    )
    out_specs = P(("groups", "expert"), None)
    return jax.shard_map(layer, mesh=mesh, in_specs=in_specs, out_specs=out_specs, check_vma=False)
```

```python
import functools

import jax
import jax.numpy as jnp
from jax import lax
from jax.experimental import pallas as pl
from jax.experimental.pallas import tpu as pltpu
from jax.sharding import PartitionSpec as P


LANES = 128
BF16 = jnp.bfloat16
F32 = jnp.float32
HBM = pl.BlockSpec(memory_space=pltpu.HBM)
VMEM = pl.BlockSpec(memory_space=pltpu.VMEM)
SMEM = pl.BlockSpec(memory_space=pltpu.SMEM)


def swap(block, mask):
    count = lax.axis_size("expert")
    return lax.ppermute(block, "expert", [(i, i ^ mask) for i in range(count)])


def picked_rows(placing, body):
    return lax.dot_general(placing, body, (((0,), (0,)), ((), ())), preferred_element_type=F32)


def slot_weights(table, station, masks, slots, cap, rows_each):
    rows = table.shape[0]
    row = lax.broadcasted_iota(jnp.int32, (rows, rows), 0)
    col = lax.broadcasted_iota(jnp.int32, (rows, rows), 1)
    earlier = (col < row) & (row // rows_each == col // rows_each)
    rank = jnp.dot(
        jnp.where(earlier, 1.0, 0.0).astype(BF16),
        jnp.where(table > 0.0, 1.0, 0.0).astype(BF16),
        preferred_element_type=F32,
    )
    base = lax.broadcasted_iota(jnp.int32, (rows, 1), 0) // rows_each * cap
    lane = lax.broadcasted_iota(jnp.int32, table.shape, 1)
    target = lax.broadcasted_iota(jnp.int32, (rows, len(masks) * slots), 1)
    weights = jnp.zeros((rows, len(masks) * slots), F32)
    for j, mask in enumerate(masks):
        pick = lane == (station ^ mask)
        share = jnp.sum(jnp.where(pick, table, 0.0), axis=1, keepdims=True)
        ranked = jnp.sum(jnp.where(pick, rank, 0.0), axis=1, keepdims=True)
        slot = base + ranked.astype(jnp.int32) + j * slots
        weights = weights + jnp.where(target == slot, share, 0.0)
    return weights


def prepare_kernel(station, *refs, peers, cap, slots, width):
    sources = refs[:5]
    heavy = refs[5]
    payload, loaded = refs[6:8]
    chosen = refs[8 : 8 + peers]
    copied = refs[8 + peers : 13 + peers]
    sems, heavy_sems = refs[-2:]
    copies = [
        pltpu.make_async_copy(source, target, sems.at[n])
        for n, (source, target) in enumerate(zip(sources, copied))
    ]
    for copy in copies:
        copy.start()
    weights = pieces_of(heavy, loaded, heavy_sems, 0)
    for copy in weights:
        copy.start()
    for copy in copies:
        copy.wait()
    tokens, gain, ids, score, pair = copied
    widened = tokens[...].astype(F32)
    meansq = jnp.mean(widened * widened, axis=-1, keepdims=True)
    normed = (widened * lax.rsqrt(meansq + 1e-06) * gain[...]).astype(BF16)
    payload[:, :width] = normed
    rows, top = ids.shape
    stations = pair.shape[1]
    shares = score[...] / jnp.sum(score[...], axis=-1, keepdims=True)
    labels = lax.broadcasted_iota(jnp.int32, (rows, stations), 1)
    named = jnp.zeros((rows, stations), F32)
    for k in range(top):
        named = named + jnp.where(ids[:, k : k + 1] == labels, shares[:, k : k + 1], 0.0)
    place = lax.broadcasted_iota(jnp.int32, (payload.shape[1] - width, stations), 0)
    moved = jnp.where(pair[...] == place, 1.0, 0.0).astype(BF16)
    table = lax.dot_general(
        named.astype(BF16), moved, (((1,), (1,)), ((), ())), preferred_element_type=F32
    )
    payload[:, width:] = table.astype(BF16)
    shared = slot_weights(table, station[0], range(1, peers + 1), slots, cap, rows)
    placed = picked_rows(jnp.where(shared > 0.0, 1.0, 0.0).astype(BF16), normed)
    for j, ref in enumerate(chosen):
        ref[...] = placed[j * slots : (j + 1) * slots].astype(BF16)
    for copy in weights:
        copy.wait()


def select_kernel(station, *refs, blocks, peers, cap, slots, width):
    payloads = refs[:blocks]
    own, tables = refs[blocks : blocks + 2]
    chosen = refs[blocks + 2 :]
    rows = payloads[0].shape[0]
    gathered = jnp.concatenate([ref[...].astype(F32) for ref in payloads], axis=0)
    table = gathered[:, width:]
    body = gathered[:, :width].astype(BF16)
    tables[...] = table
    held = own.shape[0]
    here = slot_weights(table, station[0], [0], held, cap, rows)
    away = slot_weights(table[rows:], station[0], range(1, peers + 1), slots, cap, rows)
    away = jnp.concatenate([jnp.zeros((rows, away.shape[1]), F32), away], axis=0)
    shared = jnp.concatenate([here, away], axis=1)
    placed = picked_rows(jnp.where(shared > 0.0, 1.0, 0.0).astype(BF16), body)
    own[...] = placed[:held].astype(BF16)
    for j, ref in enumerate(chosen):
        ref[...] = placed[held + j * slots : held + (j + 1) * slots].astype(BF16)


def weigh(station, tables, shares, *outs, peers, cap, rows_each):
    table = tables[...]
    held = shares.shape[1]
    shares[...] = slot_weights(table, station[0], [0], held, cap, rows_each).astype(BF16)
    for h, weights in enumerate(outs):
        folds, rows, lanes = weights.shape
        back = lanes // peers // folds
        part = table[h * rows : (h + 1) * rows]
        shared = slot_weights(
            part, station[0], range(1, peers + 1), folds * back, cap, rows_each
        )
        weights[0] = shared.astype(BF16)
        for f in range(1, folds):
            shared = jnp.concatenate(
                [jnp.zeros((rows, back), F32), shared[:, : lanes - back]], axis=1
            )
            weights[f] = shared.astype(BF16)


def activate(projected):
    half = projected.shape[1] // 2
    gate = projected[:, :half]
    return (gate / (1.0 + jnp.exp(-gate)) * projected[:, half:]).astype(BF16)


def pieces_of(weights, loaded, sems, start):
    steps = sems.shape[0]
    size = loaded.shape[0] // steps
    return [
        pltpu.make_async_copy(
            weights.at[0, pl.ds(start + s * size, size)],
            loaded.at[pl.ds(s * size, size)],
            sems.at[s],
        )
        for s in range(steps)
    ]


def load_kernel(*refs, starts):
    count = len(starts)
    copies = []
    for n, start in enumerate(starts):
        copies += pieces_of(refs[n], refs[count + n], refs[2 * count + n], start)
    for copy in copies:
        copy.start()
    for copy in copies:
        copy.wait()


def load_and_weigh_kernel(station, tables, *refs, starts, **sizes):
    count = len(starts)
    copies = []
    for n, start in enumerate(starts):
        copies += pieces_of(refs[n], refs[count + n], refs[2 * count + 3 + n], start)
    for copy in copies:
        copy.start()
    weigh(station, tables, *refs[2 * count : 2 * count + 3], **sizes)
    for copy in copies:
        copy.wait()


def hidden_of(stacked, inward):
    total = None
    start = 0
    for ref in inward:
        end = start + ref.shape[0]
        part = jnp.dot(stacked[:, start:end], ref[...], preferred_element_type=F32)
        total = part if total is None else total + part
        start = end
    return activate(total)


def expert_kernel(*refs, peers, parts, held, cap, near, far, folds, steps):
    arrived, swapped = refs[:peers], refs[peers : 2 * peers]
    own, other = refs[2 * peers : 2 * peers + 2]
    inward = refs[2 * peers + 2 : 2 * peers + 2 + parts]
    outward = refs[2 * peers + 2 + parts]
    results = refs[2 * peers + 3 + parts : -1]
    keep_far, give_far = results[:peers], results[peers : 2 * peers]
    keep_near, give_near, keep, give = results[2 * peers :]
    stacked = refs[-1]
    width = own.shape[1]
    slots = arrived[0].shape[0]
    pieces = arrived + swapped
    for p, ref in enumerate(pieces):
        stacked[p * slots : (p + 1) * slots] = ref[...]
    base = len(pieces) * slots
    early = (stacked.shape[0] - base) // 2
    slots_first = (own.shape[0] - held) // peers
    for side, ref in enumerate((own, other)):
        offset = base + side * early
        stacked[offset : offset + held] = ref[:held]
        loose = ref[held:].astype(F32)
        tight = [loose[j * slots_first : j * slots_first + cap] for j in range(peers)]
        spare = early - held - peers * cap
        if spare:
            tight.append(jnp.zeros((spare, width), F32))
        stacked[offset + held : offset + early] = jnp.concatenate(tight, axis=0).astype(BF16)
    hidden = hidden_of(stacked, inward)
    n_len = width // folds // steps
    tall = folds * far * cap
    for c in range(steps):
        cols = slice(c * n_len, (c + 1) * n_len)
        values = []
        for f in range(folds):
            start = f * (width // folds) + c * n_len
            wide = slice(start, start + n_len)
            value = jnp.dot(hidden, outward[:, wide], preferred_element_type=F32)
            keep[:, wide] = value[base : base + held]
            give[:, wide] = value[base + early : base + early + held].astype(BF16)
            values.append(value)
        for p in range(2 * peers):
            side, j = divmod(p, peers)
            first = base + side * early + held + j * cap
            distant, close = [], []
            for value in values:
                start = p * slots + (near - 1) * cap
                distant.append(value[start : start + far * cap])
                close.append(value[first : first + cap])
                close.append(value[p * slots : start])
            ref = (give_far if side else keep_far)[j]
            ref[:, cols] = jnp.concatenate(distant, axis=0).astype(ref.dtype)
            ref = give_near if side else keep_near
            ref[j * tall : (j + 1) * tall, cols] = jnp.concatenate(close, axis=0).astype(ref.dtype)


def combine_kernel(shares, weights, keep, got, *refs, peers, start):
    back = refs[:peers]
    blocks = refs[peers:]
    stacked = jnp.concatenate([ref[...] for ref in back], axis=0)
    folds, size, _ = weights.shape
    span = slice(start, start + size)
    rows = blocks[0].shape[0]
    for f in range(folds):
        cols = slice(f * stacked.shape[1], (f + 1) * stacked.shape[1])
        mixed = jnp.dot(weights[f], stacked, preferred_element_type=F32)
        local = (keep[:, cols] + got[:, cols].astype(F32)).astype(BF16)
        mixed = mixed + jnp.dot(shares[span], local, preferred_element_type=F32)
        for b, ref in enumerate(blocks):
            ref[:, cols] = mixed[b * rows : (b + 1) * rows].astype(ref.dtype)


def total_kernel(local, *refs):
    total = local[...]
    for ref in refs[:-1]:
        total = total + ref[...].astype(F32)
    refs[-1][...] = total.astype(BF16)


def call(kernel, ins, outs, scratch=(), limit=6, flops=0, moved=0):
    return pl.pallas_call(
        kernel,
        in_specs=list(ins),
        out_specs=[VMEM] * len(outs),
        out_shape=[jax.ShapeDtypeStruct(*out) for out in outs],
        scratch_shapes=list(scratch),
        cost_estimate=pl.CostEstimate(flops=flops, bytes_accessed=moved, transcendentals=0),
        compiler_params=pltpu.CompilerParams(vmem_limit_bytes=limit << 20),
    )


def layer(tokens, norm_gain, expert_ids, route_score, expert_pair, w_in, w_out):
    devices = lax.axis_size("expert")
    blocks, plane, up = shape_of(devices)
    peers = plane - 1
    stations = expert_pair.shape[0]
    rows, top = expert_ids.shape
    width = tokens.shape[1]
    half = w_out.shape[1]
    cap = min(rows, -(-rows * top // stations) + 1)
    slots_first = -(-cap // 8) * 8
    slots = -(-(blocks - 1) * cap // 8) * 8
    near = blocks // 2
    far = blocks - near
    folds = next(f for f in (1, 2, 4, 8) if f * far * cap % 8 == 0)
    packed = (folds * far * cap, width // folds)
    table = -(-stations // LANES) * LANES
    held = -(-blocks * cap // 8) * 8
    early = held + -(-peers * cap // 8) * 8
    station = (lax.axis_index("expert") // 2).astype(jnp.int32).reshape(1)
    hbm = functools.partial(pltpu.with_memory_space_constraint, memory_space=pltpu.HBM)
    w_in, w_out = hbm(w_in), hbm(w_out)
    cuts = (width // 8, width * 3 // 8, width // 2)

    inputs = (
        tokens,
        norm_gain.reshape(1, width),
        expert_ids,
        route_score,
        expert_pair.reshape(1, stations),
    )
    payload, inward0, *first = call(
        functools.partial(prepare_kernel, peers=peers, cap=cap, slots=slots_first, width=width),
        [SMEM] + [HBM] * 6,
        [((rows, width + table), BF16), ((cuts[0], 2 * half), BF16)]
        + [((slots_first, width), BF16)] * peers,
        [pltpu.VMEM(x.shape, x.dtype) for x in inputs]
        + [pltpu.SemaphoreType.DMA((5,)), pltpu.SemaphoreType.DMA((4,))],
    )(station, *[hbm(x) for x in inputs], w_in)
    middle = call(
        functools.partial(load_kernel, starts=[cuts[0]]),
        [HBM],
        [((cuts[1], 2 * half), BF16)],
        [pltpu.SemaphoreType.DMA((6,))],
    )
    (inward1,) = middle(w_in)

    column = [payload] + [swap(payload, k << up) for k in range(1, blocks)]
    first = [swap(first[j], (j + 1) << 1) for j in range(peers)]
    own, tables, *chosen = call(
        functools.partial(
            select_kernel, blocks=blocks, peers=peers, cap=cap, slots=slots, width=width
        ),
        [SMEM] + [VMEM] * blocks,
        [((held, width), BF16), ((blocks * rows, table), F32)]
        + [((slots, width), BF16)] * peers,
    )(station, *column)

    tall = packed[0]
    last = call(
        functools.partial(
            load_and_weigh_kernel,
            starts=[cuts[0] + cuts[1], 0],
            peers=peers,
            cap=cap,
            rows_each=rows,
        ),
        [SMEM, VMEM, HBM, HBM],
        [((cuts[2], 2 * half), BF16), ((half, width), BF16), ((blocks * rows, held), BF16)]
        + [((folds, far * rows, peers * tall), BF16)] * 2,
        [pltpu.SemaphoreType.DMA((8,)), pltpu.SemaphoreType.DMA((6,))],
    )
    inward2, outward, shares, weights_near, weights_far = last(station, tables, w_in, w_out)
    inward = [inward0, inward1, inward2]
    arrived = [swap(chosen[j], (j + 1) << 1) for j in range(peers)]
    own = jnp.concatenate([own] + first, axis=0)
    other = swap(own, 1)
    swapped = [swap(block, 1) for block in arrived]
    parts = len(inward)
    expert_call = call(
        functools.partial(
            expert_kernel,
            peers=peers,
            parts=parts,
            held=held,
            cap=cap,
            near=near,
            far=far,
            folds=folds,
            steps=1,
        ),
        [VMEM] * (2 * peers + 3 + parts),
        [(packed, F32)] * peers
        + [(packed, BF16)] * peers
        + [((peers * tall, packed[1]), kind) for kind in (F32, BF16)]
        + [((held, width), kind) for kind in (F32, BF16)],
        [pltpu.VMEM((2 * (peers * slots + early), width), BF16)],
        limit=20,
    )
    results = expert_call(*arrived, *swapped, own, other, *inward, outward)
    keep_near, give_near, keep, give = results[2 * peers :]
    back_far = []
    for j in range(peers):
        halves = swap(results[peers + j], 1)
        done = (results[j] + halves.astype(F32)).astype(BF16)
        back_far.append(swap(done, (j + 1) << 1))
    got_near = swap(give_near, 1)
    back_near = []
    for j in range(peers):
        span = slice(j * tall, (j + 1) * tall)
        done = (keep_near[span] + got_near[span].astype(F32)).astype(BF16)
        back_near.append(swap(done, (j + 1) << 1))
    got = swap(give, 1)
    def combine(start, weights, back, kinds):
        kernel = call(
            functools.partial(combine_kernel, peers=peers, start=start),
            [VMEM] * (4 + peers),
            [((rows, width), kind) for kind in kinds],
        )
        return kernel(shares, weights, keep, got, *back)

    summed_far = combine(near * rows, weights_far, back_far, [BF16] * far)
    summed_near = combine(0, weights_near, back_near, [F32] + [BF16] * (near - 1))
    summed = list(summed_near) + list(summed_far)
    returned = [swap(summed[k], k << up) for k in range(1, blocks)]
    (mixed,) = call(total_kernel, [VMEM] * blocks, [((rows, width), BF16)])(summed[0], *returned)
    return mixed


def shape_of(devices):
    bits = (devices // 2).bit_length() - 1
    low = bits // 2
    return 1 << (bits - low), 1 << low, low + 1


def solution(mesh):
    in_specs = (
        P(("groups", "expert"), None),
        P(),
        P(("groups", "expert"), None),
        P(("groups", "expert"), None),
        P("groups"),
        P(("groups", "expert"), None, None),
        P(("groups", "expert"), None, None),
    )
    out_specs = P(("groups", "expert"), None)
    return jax.shard_map(layer, mesh=mesh, in_specs=in_specs, out_specs=out_specs, check_vma=False)
```

```python
import functools

import jax
import jax.numpy as jnp
from jax import lax
from jax.experimental import pallas as pl
from jax.experimental.pallas import tpu as pltpu
from jax.sharding import PartitionSpec as P


LANES = 128
BF16 = jnp.bfloat16
F32 = jnp.float32
HBM = pl.BlockSpec(memory_space=pltpu.HBM)
VMEM = pl.BlockSpec(memory_space=pltpu.VMEM)
SMEM = pl.BlockSpec(memory_space=pltpu.SMEM)


def swap(block, mask):
    count = lax.axis_size("expert")
    return lax.ppermute(block, "expert", [(i, i ^ mask) for i in range(count)])


def picked_rows(placing, body):
    return lax.dot_general(placing, body, (((0,), (0,)), ((), ())), preferred_element_type=F32)


def slot_weights(table, station, masks, slots, cap, rows_each):
    rows = table.shape[0]
    row = lax.broadcasted_iota(jnp.int32, (rows, rows), 0)
    col = lax.broadcasted_iota(jnp.int32, (rows, rows), 1)
    earlier = (col < row) & (row // rows_each == col // rows_each)
    rank = jnp.dot(
        jnp.where(earlier, 1.0, 0.0).astype(BF16),
        jnp.where(table > 0.0, 1.0, 0.0).astype(BF16),
        preferred_element_type=F32,
    )
    base = lax.broadcasted_iota(jnp.int32, (rows, 1), 0) // rows_each * cap
    lane = lax.broadcasted_iota(jnp.int32, table.shape, 1)
    target = lax.broadcasted_iota(jnp.int32, (rows, len(masks) * slots), 1)
    weights = jnp.zeros((rows, len(masks) * slots), F32)
    for j, mask in enumerate(masks):
        pick = lane == (station ^ mask)
        share = jnp.sum(jnp.where(pick, table, 0.0), axis=1, keepdims=True)
        ranked = jnp.sum(jnp.where(pick, rank, 0.0), axis=1, keepdims=True)
        slot = base + ranked.astype(jnp.int32) + j * slots
        weights = weights + jnp.where(target == slot, share, 0.0)
    return weights


def prepare_kernel(station, *refs, peers, cap, slots, width):
    sources = refs[:5]
    heavy = refs[5]
    payload, loaded = refs[6:8]
    chosen = refs[8 : 8 + peers]
    copied = refs[8 + peers : 13 + peers]
    sems, heavy_sems = refs[-2:]
    copies = [
        pltpu.make_async_copy(source, target, sems.at[n])
        for n, (source, target) in enumerate(zip(sources, copied))
    ]
    for copy in copies:
        copy.start()
    weights = pieces_of(heavy, loaded, heavy_sems, 0)
    for copy in weights:
        copy.start()
    for copy in copies:
        copy.wait()
    tokens, gain, ids, score, pair = copied
    widened = tokens[...].astype(F32)
    meansq = jnp.mean(widened * widened, axis=-1, keepdims=True)
    normed = (widened * lax.rsqrt(meansq + 1e-06) * gain[...]).astype(BF16)
    payload[:, :width] = normed
    rows, top = ids.shape
    stations = pair.shape[1]
    shares = score[...] / jnp.sum(score[...], axis=-1, keepdims=True)
    labels = lax.broadcasted_iota(jnp.int32, (rows, stations), 1)
    named = jnp.zeros((rows, stations), F32)
    for k in range(top):
        named = named + jnp.where(ids[:, k : k + 1] == labels, shares[:, k : k + 1], 0.0)
    place = lax.broadcasted_iota(jnp.int32, (payload.shape[1] - width, stations), 0)
    moved = jnp.where(pair[...] == place, 1.0, 0.0).astype(BF16)
    table = lax.dot_general(
        named.astype(BF16), moved, (((1,), (1,)), ((), ())), preferred_element_type=F32
    )
    payload[:, width:] = table.astype(BF16)
    shared = slot_weights(table, station[0], range(1, peers + 1), slots, cap, rows)
    placed = picked_rows(jnp.where(shared > 0.0, 1.0, 0.0).astype(BF16), normed)
    for j, ref in enumerate(chosen):
        ref[...] = placed[j * slots : (j + 1) * slots].astype(BF16)
    for copy in weights:
        copy.wait()


def select_kernel(station, *refs, blocks, peers, cap, slots, width):
    payloads = refs[:blocks]
    own, tables = refs[blocks : blocks + 2]
    chosen = refs[blocks + 2 :]
    rows = payloads[0].shape[0]
    gathered = jnp.concatenate([ref[...].astype(F32) for ref in payloads], axis=0)
    table = gathered[:, width:]
    body = gathered[:, :width].astype(BF16)
    tables[...] = table
    held = own.shape[0]
    here = slot_weights(table, station[0], [0], held, cap, rows)
    away = slot_weights(table[rows:], station[0], range(1, peers + 1), slots, cap, rows)
    away = jnp.concatenate([jnp.zeros((rows, away.shape[1]), F32), away], axis=0)
    shared = jnp.concatenate([here, away], axis=1)
    placed = picked_rows(jnp.where(shared > 0.0, 1.0, 0.0).astype(BF16), body)
    own[...] = placed[:held].astype(BF16)
    for j, ref in enumerate(chosen):
        ref[...] = placed[held + j * slots : held + (j + 1) * slots].astype(BF16)


def weigh(station, tables, shares, *outs, peers, cap, rows_each):
    table = tables[...]
    held = shares.shape[1]
    shares[...] = slot_weights(table, station[0], [0], held, cap, rows_each).astype(BF16)
    for h, weights in enumerate(outs):
        folds, rows, lanes = weights.shape
        back = lanes // peers // folds
        part = table[h * rows : (h + 1) * rows]
        shared = slot_weights(
            part, station[0], range(1, peers + 1), folds * back, cap, rows_each
        )
        weights[0] = shared.astype(BF16)
        for f in range(1, folds):
            shared = jnp.concatenate(
                [jnp.zeros((rows, back), F32), shared[:, : lanes - back]], axis=1
            )
            weights[f] = shared.astype(BF16)


def activate(projected):
    half = projected.shape[1] // 2
    gate = projected[:, :half]
    return (gate / (1.0 + jnp.exp(-gate)) * projected[:, half:]).astype(BF16)


def pieces_of(weights, loaded, sems, start):
    steps = sems.shape[0]
    size = loaded.shape[0] // steps
    return [
        pltpu.make_async_copy(
            weights.at[0, pl.ds(start + s * size, size)],
            loaded.at[pl.ds(s * size, size)],
            sems.at[s],
        )
        for s in range(steps)
    ]


def load_kernel(*refs, starts):
    count = len(starts)
    copies = []
    for n, start in enumerate(starts):
        copies += pieces_of(refs[n], refs[count + n], refs[2 * count + n], start)
    for copy in copies:
        copy.start()
    for copy in copies:
        copy.wait()


def load_and_weigh_kernel(station, tables, *refs, starts, **sizes):
    count = len(starts)
    copies = []
    for n, start in enumerate(starts):
        copies += pieces_of(refs[n], refs[count + n], refs[2 * count + 3 + n], start)
    for copy in copies:
        copy.start()
    weigh(station, tables, *refs[2 * count : 2 * count + 3], **sizes)
    for copy in copies:
        copy.wait()


def hidden_of(stacked, inward):
    total = None
    start = 0
    for ref in inward:
        end = start + ref.shape[0]
        part = jnp.dot(stacked[:, start:end], ref[...], preferred_element_type=F32)
        total = part if total is None else total + part
        start = end
    return activate(total)


def expert_kernel(*refs, peers, parts, held, cap, near, far, folds, steps):
    arrived, swapped = refs[:peers], refs[peers : 2 * peers]
    own, other = refs[2 * peers : 2 * peers + 2]
    inward = refs[2 * peers + 2 : 2 * peers + 2 + parts]
    outward = refs[2 * peers + 2 + parts]
    results = refs[2 * peers + 3 + parts : -1]
    keep_far, give_far = results[:peers], results[peers : 2 * peers]
    keep_near, give_near, keep, give = results[2 * peers :]
    stacked = refs[-1]
    width = own.shape[1]
    slots = arrived[0].shape[0]
    pieces = arrived + swapped
    for p, ref in enumerate(pieces):
        stacked[p * slots : (p + 1) * slots] = ref[...]
    base = len(pieces) * slots
    early = (stacked.shape[0] - base) // 2
    slots_first = (own.shape[0] - held) // peers
    for side, ref in enumerate((own, other)):
        offset = base + side * early
        stacked[offset : offset + held] = ref[:held]
        loose = ref[held:].astype(F32)
        tight = [loose[j * slots_first : j * slots_first + cap] for j in range(peers)]
        spare = early - held - peers * cap
        if spare:
            tight.append(jnp.zeros((spare, width), F32))
        stacked[offset + held : offset + early] = jnp.concatenate(tight, axis=0).astype(BF16)
    hidden = hidden_of(stacked, inward)
    n_len = width // folds // steps
    tall = folds * far * cap
    for c in range(steps):
        cols = slice(c * n_len, (c + 1) * n_len)
        values = []
        for f in range(folds):
            start = f * (width // folds) + c * n_len
            wide = slice(start, start + n_len)
            value = jnp.dot(hidden, outward[:, wide], preferred_element_type=F32)
            keep[:, wide] = value[base : base + held]
            give[:, wide] = value[base + early : base + early + held].astype(BF16)
            values.append(value)
        for p in range(2 * peers):
            side, j = divmod(p, peers)
            first = base + side * early + held + j * cap
            distant, close = [], []
            for value in values:
                start = p * slots + (near - 1) * cap
                distant.append(value[start : start + far * cap])
                close.append(value[first : first + cap])
                close.append(value[p * slots : start])
            ref = (give_far if side else keep_far)[j]
            ref[:, cols] = jnp.concatenate(distant, axis=0).astype(ref.dtype)
            ref = give_near if side else keep_near
            ref[j * tall : (j + 1) * tall, cols] = jnp.concatenate(close, axis=0).astype(ref.dtype)


def combine_kernel(shares, weights, keep, got, *refs, peers, start):
    back = refs[:peers]
    blocks = refs[peers:]
    stacked = jnp.concatenate([ref[...] for ref in back], axis=0)
    folds, size, _ = weights.shape
    span = slice(start, start + size)
    rows = blocks[0].shape[0]
    for f in range(folds):
        cols = slice(f * stacked.shape[1], (f + 1) * stacked.shape[1])
        mixed = jnp.dot(weights[f], stacked, preferred_element_type=F32)
        local = (keep[:, cols] + got[:, cols].astype(F32)).astype(BF16)
        mixed = mixed + jnp.dot(shares[span], local, preferred_element_type=F32)
        for b, ref in enumerate(blocks):
            ref[:, cols] = mixed[b * rows : (b + 1) * rows].astype(ref.dtype)


def total_kernel(local, *refs):
    total = local[...]
    for ref in refs[:-1]:
        total = total + ref[...].astype(F32)
    refs[-1][...] = total.astype(BF16)


def call(kernel, ins, outs, scratch=(), limit=6, flops=0, moved=0):
    return pl.pallas_call(
        kernel,
        in_specs=list(ins),
        out_specs=[VMEM] * len(outs),
        out_shape=[jax.ShapeDtypeStruct(*out) for out in outs],
        scratch_shapes=list(scratch),
        cost_estimate=pl.CostEstimate(flops=flops, bytes_accessed=moved, transcendentals=0),
        compiler_params=pltpu.CompilerParams(vmem_limit_bytes=limit << 20),
    )


def layer(tokens, norm_gain, expert_ids, route_score, expert_pair, w_in, w_out):
    devices = lax.axis_size("expert")
    blocks, plane, up = shape_of(devices)
    peers = plane - 1
    stations = expert_pair.shape[0]
    rows, top = expert_ids.shape
    width = tokens.shape[1]
    half = w_out.shape[1]
    cap = min(rows, -(-rows * top // stations) + 1)
    slots_first = -(-cap // 8) * 8
    slots = -(-(blocks - 1) * cap // 8) * 8
    near = blocks // 2
    far = blocks - near
    folds = next(f for f in (1, 2, 4, 8) if f * far * cap % 8 == 0)
    packed = (folds * far * cap, width // folds)
    table = -(-stations // LANES) * LANES
    held = -(-blocks * cap // 8) * 8
    early = held + -(-peers * cap // 8) * 8
    station = (lax.axis_index("expert") // 2).astype(jnp.int32).reshape(1)
    hbm = functools.partial(pltpu.with_memory_space_constraint, memory_space=pltpu.HBM)
    w_in, w_out = hbm(w_in), hbm(w_out)
    cuts = (width // 16, width // 4, width * 11 // 16)

    inputs = (
        tokens,
        norm_gain.reshape(1, width),
        expert_ids,
        route_score,
        expert_pair.reshape(1, stations),
    )
    payload, inward0, *first = call(
        functools.partial(prepare_kernel, peers=peers, cap=cap, slots=slots_first, width=width),
        [SMEM] + [HBM] * 6,
        [((rows, width + table), BF16), ((cuts[0], 2 * half), BF16)]
        + [((slots_first, width), BF16)] * peers,
        [pltpu.VMEM(x.shape, x.dtype) for x in inputs]
        + [pltpu.SemaphoreType.DMA((5,)), pltpu.SemaphoreType.DMA((4,))],
    )(station, *[hbm(x) for x in inputs], w_in)
    middle = call(
        functools.partial(load_kernel, starts=[cuts[0]]),
        [HBM],
        [((cuts[1], 2 * half), BF16)],
        [pltpu.SemaphoreType.DMA((4,))],
    )
    (inward1,) = middle(w_in)

    column = [payload] + [swap(payload, k << up) for k in range(1, blocks)]
    first = [swap(first[j], (j + 1) << 1) for j in range(peers)]
    own, tables, *chosen = call(
        functools.partial(
            select_kernel, blocks=blocks, peers=peers, cap=cap, slots=slots, width=width
        ),
        [SMEM] + [VMEM] * blocks,
        [((held, width), BF16), ((blocks * rows, table), F32)]
        + [((slots, width), BF16)] * peers,
    )(station, *column)

    tall = packed[0]
    last = call(
        functools.partial(
            load_and_weigh_kernel,
            starts=[cuts[0] + cuts[1], 0],
            peers=peers,
            cap=cap,
            rows_each=rows,
        ),
        [SMEM, VMEM, HBM, HBM],
        [((cuts[2], 2 * half), BF16), ((half, width), BF16), ((blocks * rows, held), BF16)]
        + [((folds, far * rows, peers * tall), BF16)] * 2,
        [pltpu.SemaphoreType.DMA((8,)), pltpu.SemaphoreType.DMA((6,))],
    )
    inward2, outward, shares, weights_near, weights_far = last(station, tables, w_in, w_out)
    inward = [inward0, inward1, inward2]
    arrived = [swap(chosen[j], (j + 1) << 1) for j in range(peers)]
    own = jnp.concatenate([own] + first, axis=0)
    other = swap(own, 1)
    swapped = [swap(block, 1) for block in arrived]
    parts = len(inward)
    expert_call = call(
        functools.partial(
            expert_kernel,
            peers=peers,
            parts=parts,
            held=held,
            cap=cap,
            near=near,
            far=far,
            folds=folds,
            steps=4,
        ),
        [VMEM] * (2 * peers + 3 + parts),
        [(packed, F32)] * peers
        + [(packed, BF16)] * peers
        + [((peers * tall, packed[1]), kind) for kind in (F32, BF16)]
        + [((held, width), kind) for kind in (F32, BF16)],
        [pltpu.VMEM((2 * (peers * slots + early), width), BF16)],
        limit=20,
    )
    results = expert_call(*arrived, *swapped, own, other, *inward, outward)
    keep_near, give_near, keep, give = results[2 * peers :]
    back_far = []
    for j in range(peers):
        halves = swap(results[peers + j], 1)
        done = (results[j] + halves.astype(F32)).astype(BF16)
        back_far.append(swap(done, (j + 1) << 1))
    got_near = swap(give_near, 1)
    back_near = []
    for j in range(peers):
        span = slice(j * tall, (j + 1) * tall)
        done = (keep_near[span] + got_near[span].astype(F32)).astype(BF16)
        back_near.append(swap(done, (j + 1) << 1))
    got = swap(give, 1)
    def combine(start, weights, back, kinds):
        kernel = call(
            functools.partial(combine_kernel, peers=peers, start=start),
            [VMEM] * (4 + peers),
            [((rows, width), kind) for kind in kinds],
        )
        return kernel(shares, weights, keep, got, *back)

    summed_far = combine(near * rows, weights_far, back_far, [BF16] * far)
    summed_near = combine(0, weights_near, back_near, [F32] + [BF16] * (near - 1))
    summed = list(summed_near) + list(summed_far)
    returned = [swap(summed[k], k << up) for k in range(1, blocks)]
    (mixed,) = call(total_kernel, [VMEM] * blocks, [((rows, width), BF16)])(summed[0], *returned)
    return mixed


def shape_of(devices):
    bits = (devices // 2).bit_length() - 1
    low = bits // 2
    return 1 << (bits - low), 1 << low, low + 1


def solution(mesh):
    in_specs = (
        P(("groups", "expert"), None),
        P(),
        P(("groups", "expert"), None),
        P(("groups", "expert"), None),
        P("groups"),
        P(("groups", "expert"), None, None),
        P(("groups", "expert"), None, None),
    )
    out_specs = P(("groups", "expert"), None)
    return jax.shard_map(layer, mesh=mesh, in_specs=in_specs, out_specs=out_specs, check_vma=False)
```
